128 devices in a mesh: gx: 8 (over x, core), gy: 16 (over z, y).
Axes of the slice: x: 4, y: 4, z: 4, core: 2. Of those that a mesh axis runs over, the one named last changes fastest.
Arguments:
- record_keys: int32 [131072], P(('gx', 'gy')), may hold values from 0 to 16777215
- payloads: int32 [131072], P(('gx', 'gy')), may hold values from 0 to 16777215
Outputs:
- sorted_keys: int32 [245760], P(('gx', 'gy'))
- sorted_payloads: int32 [245760], P(('gx', 'gy'))
- bucket_sizes: int32 [128], P(('gx', 'gy'))
- bucket_digest: int32 [128], P(('gx', 'gy'))
The draws below stay inside these ranges and needn't reach their ends.
All inputs are finite; a program needn't handle non-finite values.
Results may differ from the reference program's by a relative error of at most 0.000001.
Values may be sent and summed in bfloat16 or wider, within the bound.
A program may use at most 64 MiB of HBM per device.

```python
import math
import jax
import jax.numpy as jnp
import numpy as np
from jax import lax

KEYS_DEV = 1024
KEY_RANGE = 16777216
BUCKETS = 128
TOTAL = 131072
GROUP = 8
BUCKET_CAP = 1920


def plant(array, key, least, top_value):
    place = [jax.random.randint(jax.random.fold_in(key, axis), (), 0, length) for axis, length in enumerate(array.shape)]
    main_axis = array.shape.index(max(array.shape))
    neighbour = place[:main_axis] + [(place[main_axis] + 1) % array.shape[main_axis]] + place[main_axis + 1:]
    return array.at[tuple(place)].set(least).at[tuple(neighbour)].set(top_value)


def ranked_wide(rng, dims, amount, lean):
    portions = [min(1 << octave, amount + 1 - (1 << octave)) * (1 << 20) // math.isqrt((1 << octave) ** lean) + 1 for octave in range((amount + 1).bit_length()) if 1 << octave <= amount]
    deviation = 1 + sum(portions) // (1 << 30)
    listing = np.cumsum(np.array([max(1, weight // deviation) for weight in portions]))
    pick = jax.random.randint(jax.random.fold_in(rng, 1), dims, 0, int(listing[len(portions) - 1]))
    start = jnp.left_shift(1, jnp.searchsorted(jnp.asarray(listing, jnp.int32), pick, side="right").astype(jnp.int32))
    standing = start - 1 + jax.random.randint(jax.random.fold_in(rng, 4), dims, 0, 1 << 30) % jnp.minimum(start, amount + 1 - start)
    return jax.random.permutation(jax.random.fold_in(rng, 2), amount)[standing].astype(jnp.int32)


def setup_inputs(seed: int = 0) -> dict:
    seeds = jax.random.split(jax.random.key(seed), 3)
    return {
        "record_keys": plant(ranked_wide(seeds[0], (TOTAL,), KEY_RANGE, 2), jax.random.fold_in(seeds[0], 3), 0, KEY_RANGE - 1).astype(jnp.int32),
        "payloads": plant(jax.random.randint(seeds[1], (TOTAL,), 0, KEY_RANGE), jax.random.fold_in(seeds[1], 1), 0, KEY_RANGE - 1).astype(jnp.int32),
    }


def reference(record_keys, payloads):
    places = lax.iota(jnp.int32, TOTAL)
    block_keys, block_places = lax.sort(
        (record_keys.reshape(BUCKETS, KEYS_DEV), places.reshape(BUCKETS, KEYS_DEV)),
        dimension=1, num_keys=2)
    sample_keys = block_keys.reshape(BUCKETS, BUCKETS, GROUP)[:, :, GROUP - 1].reshape(-1)
    sample_places = block_places.reshape(BUCKETS, BUCKETS, GROUP)[:, :, GROUP - 1].reshape(-1)
    sample_keys, sample_places = lax.sort((sample_keys, sample_places), num_keys=2)
    split_places = sample_places.reshape(BUCKETS, BUCKETS)[:BUCKETS - 1, BUCKETS - 1]
    order_keys, order_places, order_values = lax.sort((record_keys, places, payloads), num_keys=2)
    rank_of = lax.sort((order_places, places), num_keys=1)[1]
    split_ranks = rank_of[split_places].astype(jnp.int32)
    begins = jnp.concatenate([jnp.zeros((1,), jnp.int32), split_ranks + 1])
    stop_at = jnp.concatenate([split_ranks + 1, jnp.full((1,), TOTAL, jnp.int32)])
    lengths = stop_at - begins
    offsets = lax.iota(jnp.int32, BUCKET_CAP)
    take_at = jnp.minimum(begins[:, None] + offsets[None, :], TOTAL - 1)
    filled = offsets[None, :] < lengths[:, None]
    grid_keys = jnp.where(filled, order_keys[take_at], -1)
    grid_values = jnp.where(filled, order_values[take_at], -1)
    mixed = (grid_keys + 3 * grid_values + 5 * offsets[None, :]) % 1024
    digest = jnp.sum(jnp.where(filled, 2 * mixed - 1023, 0), axis=1).astype(jnp.int32)
    return grid_keys.reshape(-1), grid_values.reshape(-1), lengths, digest
```

```python
import functools

import jax
import jax.numpy as jnp
from jax import lax
from jax.experimental import pallas as pl
from jax.experimental.pallas import tpu as pltpu
from jax.sharding import PartitionSpec as P

MESH = pl.DeviceIdType.MESH
LANES = 128
SUBS = 8
CHUNK = 256
CHUNKS = 3
BIG = 1 << 24
f32, bf16, i32 = jnp.float32, jnp.bfloat16, jnp.int32


def iota(shape, dim):
    return lax.broadcasted_iota(i32, shape, dim)


def row(x, s):
    return jnp.broadcast_to(x[s : s + 1, :], (SUBS, LANES))


def pieces(x):
    return [x & (CHUNK - 1), (x >> 8) & (CHUNK - 1), x >> 16]


def joined(parts):
    parts = [p.astype(i32) for p in parts]
    return parts[0] + (parts[1] << 8) + (parts[2] << 16)


def placed(rows, his, los, count):
    left, right = [], []
    for (keys, values), hi, lo in zip(rows, his, los):
        parts = [p.astype(f32) for p in pieces(keys) + pieces(values)]
        for s in range(SUBS):
            onehot = jnp.broadcast_to(lo[s : s + 1, :], (LANES, LANES)) == iota((LANES, LANES), 0)
            right.append(jnp.where(onehot, 1.0, 0.0).astype(bf16))
            column = []
            at = jnp.broadcast_to(hi[s : s + 1, :], (count, LANES)) == iota((count, LANES), 0)
            for p in parts:
                column.append(jnp.where(at, jnp.broadcast_to(p[s : s + 1, :], (count, LANES)), 0.0))
            left.append(jnp.concatenate(column, axis=0).astype(bf16))
    left = jnp.concatenate(left, axis=1)
    right = jnp.concatenate(right, axis=1)
    out = lax.dot_general(left, right, (((1,), (1,)), ((), ())), preferred_element_type=f32)
    out = [out[c * count : (c + 1) * count, :] for c in range(2 * CHUNKS)]
    return joined(out[:CHUNKS]), joined(out[CHUNKS:])


def sublane_sums(accs):
    return jnp.concatenate([jnp.sum(a, axis=0, keepdims=True) for a in accs], axis=0)


STEP = 16


def block_ranks(keys):
    subs, lanes = iota((SUBS, LANES), 0), iota((SUBS, LANES), 1)
    rows = [row(keys, s) + jnp.where(subs < s, 1, 0) for s in range(SUBS)]

    def body(t, carry):
        turned, accs, ties = carry
        accs = list(accs)
        for m in range(STEP):
            one = jnp.broadcast_to(turned[:, m : m + 1], (SUBS, LANES))
            for s in range(SUBS):
                accs[s] = accs[s] + jnp.where(one < rows[s], 1, 0)
            ties = ties + jnp.where((one == keys) & (lanes > t * STEP + m), 1, 0)
        return pltpu.roll(turned, LANES - STEP, 1), tuple(accs), ties

    zero = jnp.zeros((SUBS, LANES), i32)
    _, accs, ties = lax.fori_loop(0, LANES // STEP, body, (keys, (zero,) * SUBS, zero))
    return sublane_sums(accs) + ties


def candidate_ranks(halves):
    subs, lanes = iota((SUBS, LANES), 0), iota((SUBS, LANES), 1)
    rows = [[row(k, s) for s in range(SUBS)] for k in halves]
    zero = jnp.zeros((SUBS, LANES), i32)
    accs = [[zero] * SUBS for _ in halves]
    for source, keys in enumerate(halves):

        def body(t, carry, source=source):
            turned, accs = carry
            accs = [list(a) for a in accs]
            for m in range(STEP):
                one = jnp.broadcast_to(turned[:, m : m + 1], (SUBS, LANES))
                for target in range(2):
                    less = one
                    if target == source:
                        less = one - jnp.where(lanes > t * STEP + m, 1, 0)
                    elif target > source:
                        less = one - 1
                    for s in range(SUBS):
                        accs[target][s] = accs[target][s] + jnp.where(less < rows[target][s], 1, 0)
            return pltpu.roll(turned, LANES - STEP, 1), tuple(tuple(a) for a in accs)

        _, accs = lax.fori_loop(0, LANES // STEP, body, (keys, tuple(tuple(a) for a in accs)))
    ranks = []
    for keys, acc in zip(halves, accs):
        ties = zero
        for d in range(1, SUBS):
            ties = ties + jnp.where((pltpu.roll(keys, d, 0) == keys) & (subs >= d), 1, 0)
        ranks.append(sublane_sums(acc) + ties)
    return ranks


def sorted_block(keys, values):
    rank = block_ranks(keys)
    return placed([(keys, values)], [rank & (SUBS - 1)], [rank >> 3], SUBS)


def gather_kernel(xs, planes, keys_ref, values_ref, out_ref, block, local_sem, send_sem, recv_sem, give_sem, take_sem):
    gx, gy = lax.axis_index("gx"), lax.axis_index("gy")
    x, core = gx // 2, gx % 2
    partner = x * 2 + (1 - core)
    barrier = pltpu.get_barrier_semaphore()

    def others():
        for dx in range(xs):
            for dy in range(planes):
                if dx or dy:
                    yield dx, dy

    def device(dx, dy):
        return ((x + dx) % xs) * 2 + core, (gy + dy) % planes

    for dx, dy in others():
        pl.semaphore_signal(barrier, inc=1, device_id=device(dx, dy), device_id_type=MESH)
    pl.semaphore_signal(barrier, inc=1, device_id=(partner, gy), device_id_type=MESH)

    keys, values = sorted_block(keys_ref[...], values_ref[...])
    block[0:SUBS, :] = keys
    block[SUBS : 2 * SUBS, :] = values
    pl.semaphore_wait(barrier, xs * planes)

    me = gx * planes + gy
    mine = pltpu.make_async_copy(block, out_ref.at[me], local_sem)
    mine.start()
    sends = []
    for dx, dy in others():
        copy = pltpu.make_async_remote_copy(
            src_ref=block,
            dst_ref=out_ref.at[me],
            send_sem=send_sem,
            recv_sem=recv_sem.at[(xs - dx) % xs],
            device_id=device(dx, dy),
            device_id_type=MESH,
        )
        copy.start()
        sends.append(copy)
    mine.wait()
    gives = []
    for dx in range(xs):
        at = pl.multiple_of((((x + dx) % xs) * 2 + core) * planes, planes)
        count = planes if dx else planes - 1
        arrived = out_ref.at[pl.ds(at, count)]
        pltpu.make_async_copy(arrived, arrived, recv_sem.at[dx]).wait()
        group = out_ref.at[pl.ds(at, planes)]
        give = pltpu.make_async_remote_copy(
            src_ref=group,
            dst_ref=group,
            send_sem=give_sem.at[dx],
            recv_sem=take_sem.at[dx],
            device_id=(partner, gy),
            device_id_type=MESH,
        )
        give.start()
        gives.append(give)
    sent = out_ref.at[pl.ds(0, xs * planes - 1)]
    pltpu.make_async_copy(sent, sent, send_sem).wait()
    for give in gives:
        give.wait()


def splitter_key(samples_ref, wanted):
    subs = iota((SUBS, LANES), 0)
    base = [jnp.zeros((SUBS, LANES), i32) for _ in wanted]
    for shift in range(21, -1, -3):
        tests = [b + ((subs + 1) << shift) for b in base]
        zero = jnp.zeros((SUBS, LANES), i32)

        def body(t, accs):
            accs = list(accs)
            for r in range(SUBS):
                one = jnp.broadcast_to(samples_ref[pl.ds(t * SUBS + r, 1), :], (SUBS, LANES))
                for n in range(len(tests)):
                    accs[n] = accs[n] + jnp.where(one < tests[n], 1, 0)
            return tuple(accs)

        accs = lax.fori_loop(0, LANES // SUBS, body, (zero,) * len(wanted))
        for n in range(len(wanted)):
            below = jnp.sum(accs[n].astype(f32), axis=1, keepdims=True)
            passed = jnp.where((below < wanted[n].astype(f32)) & (subs[:, :1] < SUBS - 1), 1, 0)
            digit = jnp.sum(passed, axis=0, keepdims=True)
            base[n] = base[n] + (jnp.broadcast_to(digit, (SUBS, LANES)) << shift)
    return base


def bucket_kernel(blocks_ref, keys_out, values_out, info_out, samples_ref, turn_ref, in_ref):
    devices = blocks_ref.shape[0]
    d = lax.axis_index("gx") * lax.axis_size("gy") + lax.axis_index("gy")
    square = (LANES, LANES)
    samples_ref[...] = blocks_ref[:, SUBS - 1, :]
    wanted = [d * LANES, (d + 1) * LANES]
    low, high = splitter_key(samples_ref, wanted)
    high = jnp.where(d == devices - 1, BIG, high)
    samples = samples_ref[...]
    ends = [jnp.broadcast_to(k[:1, :], square) for k in (low, high)]
    ones = jnp.ones(square, bf16)
    below = jnp.where(iota(square, 1) < iota(square, 0), 1.0, 0.0).astype(bf16)

    def mm(a, b):
        return jnp.dot(a, b, preferred_element_type=f32)

    masks = []
    for k in ends:
        masks += [samples < k, samples <= k]
    counts = mm(jnp.concatenate([jnp.where(m, 1.0, 0.0).astype(bf16) for m in masks], axis=0), ones)
    counts = [counts[n * LANES : (n + 1) * LANES, :] for n in range(4)]
    taken, tied = [], []
    for n in range(2):
        lt, le = counts[2 * n], counts[2 * n + 1]
        equal = le - lt
        before = mm(below, equal.astype(bf16))
        total = mm(ones, lt.astype(bf16))
        left = jnp.asarray(wanted[n], f32) - total - before
        taken.append(lt + jnp.clip(left, 0.0, equal))
        tied.append(jnp.where(left > equal, 1, 0))
    first = taken[0]
    number = jnp.minimum(taken[1], LANES - 1.0) - first + 1.0
    start = mm(below, number.astype(bf16)).astype(i32)
    number, first, last = number.astype(i32), first.astype(i32), taken[1].astype(i32)
    lanes = iota(square, 1)
    turn_ref[...] = (lanes - (start - first)) & (LANES - 1)
    codes = []
    for h in range(2):
        m = lanes + h * LANES
        inside = (m >= start) & (m < start + number)
        in_ref[h] = jnp.where(inside, 1, 0)
        code = jnp.where(inside, 16, 0)
        code = code + jnp.where(inside & (m == start), 1 + tied[0], 0)
        code = code + jnp.where(inside & (m == start + last - first), 4 * (1 + tied[1]), 0)
        codes.append(code.astype(f32).astype(bf16))
    codes = mm(jnp.ones((SUBS, LANES), bf16), jnp.concatenate(codes, axis=1)).astype(i32)

    zero = jnp.zeros((SUBS, LANES), i32)

    def body(t, carry):
        carry = list(carry)
        for r in range(SUBS):
            b = t * SUBS + r
            turn = jnp.broadcast_to(turn_ref[pl.ds(b, 1), :], (SUBS, LANES))
            for c in range(2):
                tile = blocks_ref[b, c * SUBS : (c + 1) * SUBS, :]
                tile = jnp.take_along_axis(tile, turn, axis=1, mode="promise_in_bounds")
                for h in range(2):
                    inside = jnp.broadcast_to(in_ref[h, pl.ds(b, 1), :], (SUBS, LANES)) > 0
                    carry[2 * c + h] = jnp.where(inside, tile, carry[2 * c + h])
        return tuple(carry)

    k0, k1, v0, v1 = lax.fori_loop(0, devices // SUBS, body, (zero,) * 4)
    keys, valid = [], []
    for h, k in enumerate((k0, k1)):
        code = codes[:, h * LANES : (h + 1) * LANES]
        is_low, is_high = code & 3, (code >> 2) & 3
        ok = code >= 16
        ok = ok & ((is_low == 0) | (k >= low + is_low - 1))
        ok = ok & ((is_high == 0) | (k < high + is_high - 1))
        valid.append(jnp.where(ok, 1, 0))
        keys.append(jnp.where(ok, k, BIG))
    size = jnp.sum(jnp.sum(valid[0] + valid[1], axis=1, keepdims=True), axis=0, keepdims=True)
    ranks = candidate_ranks(keys)
    count = 2 * SUBS
    keys, values = placed(
        [(keys[0], v0), (keys[1], v1)], [r >> 7 for r in ranks], [r & (LANES - 1) for r in ranks], count
    )
    rank = iota((count, LANES), 0) * LANES + iota((count, LANES), 1)
    filled = rank < size
    keys = jnp.where(filled, keys, -1)
    values = jnp.where(filled, values, -1)
    keys_out[...] = keys[: keys_out.shape[0], :]
    values_out[...] = values[: values_out.shape[0], :]
    mixed = (keys + 3 * values + 5 * rank) & 1023
    digest = jnp.where(filled, 2 * mixed - 1023, 0)
    digest = jnp.sum(jnp.sum(digest, axis=1, keepdims=True), axis=0, keepdims=True)
    sub = iota((SUBS, LANES), 0)
    info_out[...] = jnp.where(sub == 0, size, digest)


def gathered(keys, values, xs, planes):
    blocks = 2 * xs * planes
    return pl.pallas_call(
        functools.partial(gather_kernel, xs, planes),
        out_shape=jax.ShapeDtypeStruct((blocks, 2 * SUBS, LANES), i32),
        in_specs=[pl.BlockSpec(memory_space=pltpu.VMEM)] * 2,
        out_specs=pl.BlockSpec(memory_space=pl.ANY),
        scratch_shapes=[
            pltpu.VMEM((2 * SUBS, LANES), i32),
            pltpu.SemaphoreType.DMA,
            pltpu.SemaphoreType.DMA,
            pltpu.SemaphoreType.DMA((xs,)),
            pltpu.SemaphoreType.DMA((xs,)),
            pltpu.SemaphoreType.DMA((xs,)),
        ],
        compiler_params=pltpu.CompilerParams(collective_id=0, has_side_effects=True),
        name="gather_blocks",
    )(keys, values)


def bucket(blocks, rows):
    devices = blocks.shape[0]
    return pl.pallas_call(
        bucket_kernel,
        out_shape=(
            jax.ShapeDtypeStruct((rows, LANES), i32),
            jax.ShapeDtypeStruct((rows, LANES), i32),
            jax.ShapeDtypeStruct((SUBS, LANES), i32),
        ),
        in_specs=[pl.BlockSpec(memory_space=pltpu.VMEM)],
        out_specs=[pl.BlockSpec(memory_space=pltpu.VMEM)] * 3,
        scratch_shapes=[
            pltpu.VMEM((devices, LANES), i32),
            pltpu.VMEM((devices, LANES), i32),
            pltpu.VMEM((2, devices, LANES), i32),
        ],
        name="make_bucket",
    )(blocks)


def solution(mesh):
    gx, gy = mesh.shape["gx"], mesh.shape["gy"]

    def shards(record_keys, payloads):
        keys = record_keys.reshape(SUBS, LANES)
        values = payloads.reshape(SUBS, LANES)
        blocks = gathered(keys, values, gx // 2, gy)
        rows = (2 * record_keys.shape[0] - gx * gy) // LANES
        sorted_keys, sorted_values, info = bucket(blocks, rows)
        return (sorted_keys.reshape(-1), sorted_values.reshape(-1), info[0, :1], info[1, :1])

    spec = P(("gx", "gy"))
    return jax.shard_map(shards, mesh=mesh, in_specs=(spec,) * 2, out_specs=(spec,) * 4, check_vma=False)
```

```python
import functools

import jax
import jax.numpy as jnp
from jax import lax
from jax.experimental import pallas as pl
from jax.experimental.pallas import tpu as pltpu
from jax.sharding import PartitionSpec as P

MESH = pl.DeviceIdType.MESH
LANES = 128
SUBS = 8
CHUNK = 256
CHUNKS = 3
BIG = 1 << 24
f32, bf16, i32 = jnp.float32, jnp.bfloat16, jnp.int32


def iota(shape, dim):
    return lax.broadcasted_iota(i32, shape, dim)


def row(x, s):
    return jnp.broadcast_to(x[s : s + 1, :], (SUBS, LANES))


def pieces(x):
    return [x & (CHUNK - 1), (x >> 8) & (CHUNK - 1), x >> 16]


def joined(parts):
    parts = [p.astype(i32) for p in parts]
    return parts[0] + (parts[1] << 8) + (parts[2] << 16)


def placed(rows, his, los, count):
    left, right = [], []
    for (keys, values), hi, lo in zip(rows, his, los):
        parts = [p.astype(f32) for p in pieces(keys) + pieces(values)]
        for s in range(SUBS):
            onehot = jnp.broadcast_to(lo[s : s + 1, :], (LANES, LANES)) == iota((LANES, LANES), 0)
            right.append(jnp.where(onehot, 1.0, 0.0).astype(bf16))
            column = []
            at = jnp.broadcast_to(hi[s : s + 1, :], (count, LANES)) == iota((count, LANES), 0)
            for p in parts:
                column.append(jnp.where(at, jnp.broadcast_to(p[s : s + 1, :], (count, LANES)), 0.0))
            left.append(jnp.concatenate(column, axis=0).astype(bf16))
    left = jnp.concatenate(left, axis=1)
    right = jnp.concatenate(right, axis=1)
    out = lax.dot_general(left, right, (((1,), (1,)), ((), ())), preferred_element_type=f32)
    out = [out[c * count : (c + 1) * count, :] for c in range(2 * CHUNKS)]
    return joined(out[:CHUNKS]), joined(out[CHUNKS:])


def sublane_sums(accs):
    return jnp.concatenate([jnp.sum(a, axis=0, keepdims=True) for a in accs], axis=0)


STEP = 16


def block_ranks(keys):
    subs, lanes = iota((SUBS, LANES), 0), iota((SUBS, LANES), 1)
    rows = [row(keys, s) + jnp.where(subs < s, 1, 0) for s in range(SUBS)]

    def body(t, carry):
        turned, accs, ties = carry
        accs = list(accs)
        for m in range(STEP):
            one = jnp.broadcast_to(turned[:, m : m + 1], (SUBS, LANES))
            for s in range(SUBS):
                accs[s] = accs[s] + jnp.where(one < rows[s], 1, 0)
            ties = ties + jnp.where((one == keys) & (lanes > t * STEP + m), 1, 0)
        return pltpu.roll(turned, LANES - STEP, 1), tuple(accs), ties

    zero = jnp.zeros((SUBS, LANES), i32)
    _, accs, ties = lax.fori_loop(0, LANES // STEP, body, (keys, (zero,) * SUBS, zero))
    return sublane_sums(accs) + ties


def candidate_ranks(halves):
    subs, lanes = iota((SUBS, LANES), 0), iota((SUBS, LANES), 1)
    rows = [[row(k, s) for s in range(SUBS)] for k in halves]
    zero = jnp.zeros((SUBS, LANES), i32)
    accs = [[zero] * SUBS for _ in halves]
    for source, keys in enumerate(halves):

        def body(t, carry, source=source):
            turned, accs = carry
            accs = [list(a) for a in accs]
            for m in range(STEP):
                one = jnp.broadcast_to(turned[:, m : m + 1], (SUBS, LANES))
                for target in range(2):
                    less = one
                    if target == source:
                        less = one - jnp.where(lanes > t * STEP + m, 1, 0)
                    elif target > source:
                        less = one - 1
                    for s in range(SUBS):
                        accs[target][s] = accs[target][s] + jnp.where(less < rows[target][s], 1, 0)
            return pltpu.roll(turned, LANES - STEP, 1), tuple(tuple(a) for a in accs)

        _, accs = lax.fori_loop(0, LANES // STEP, body, (keys, tuple(tuple(a) for a in accs)))
    ranks = []
    for keys, acc in zip(halves, accs):
        ties = zero
        for d in range(1, SUBS):
            ties = ties + jnp.where((pltpu.roll(keys, d, 0) == keys) & (subs >= d), 1, 0)
        ranks.append(sublane_sums(acc) + ties)
    return ranks


def sorted_block(keys, values):
    rank = block_ranks(keys)
    return placed([(keys, values)], [rank & (SUBS - 1)], [rank >> 3], SUBS)


def gather_kernel(
    xs, planes, keys_ref, values_ref, found_ref, block, blocks, samples, turns, inside, send_sem, recv_sem, give_sem, take_sem
):
    gx, gy = lax.axis_index("gx"), lax.axis_index("gy")
    x, core = gx // 2, gx % 2
    partner = x * 2 + (1 - core)
    barrier = pltpu.get_barrier_semaphore()

    def others():
        for dx in range(xs):
            for dy in range(planes):
                if dx or dy:
                    yield dx, dy

    def device(dx, dy):
        return ((x + dx) % xs) * 2 + core, (gy + dy) % planes

    for dx, dy in others():
        pl.semaphore_signal(barrier, inc=1, device_id=device(dx, dy), device_id_type=MESH)
    pl.semaphore_signal(barrier, inc=1, device_id=(partner, gy), device_id_type=MESH)

    me = gx * planes + gy
    keys, values = sorted_block(keys_ref[...], values_ref[...])
    for ref in (block, blocks.at[me]):
        ref[0:SUBS, :] = keys
        ref[SUBS : 2 * SUBS, :] = values
    pl.semaphore_wait(barrier, xs * planes)

    for dx, dy in others():
        pltpu.make_async_remote_copy(
            src_ref=block,
            dst_ref=blocks.at[me],
            send_sem=send_sem,
            recv_sem=recv_sem.at[(xs - dx) % xs],
            device_id=device(dx, dy),
            device_id_type=MESH,
        ).start()
    gives = []
    for dx in range(xs):
        at = pl.multiple_of((((x + dx) % xs) * 2 + core) * planes, planes)
        count = planes if dx else planes - 1
        arrived = blocks.at[pl.ds(at, count)]
        pltpu.make_async_copy(arrived, arrived, recv_sem.at[dx]).wait()
        group = blocks.at[pl.ds(at, planes)]
        give = pltpu.make_async_remote_copy(
            src_ref=group,
            dst_ref=group,
            send_sem=give_sem.at[dx],
            recv_sem=take_sem.at[dx],
            device_id=(partner, gy),
            device_id_type=MESH,
        )
        give.start()
        gives.append(give)
    for give in gives:
        give.wait_recv()
    keys, values = select(blocks, samples, turns, inside)
    for n, tile in enumerate(keys + values):
        found_ref[n * SUBS : (n + 1) * SUBS, :] = tile
    sent = blocks.at[pl.ds(0, xs * planes - 1)]
    pltpu.make_async_copy(sent, sent, send_sem).wait()
    for give in gives:
        give.wait_send()


def splitter_key(samples_ref, wanted):
    subs = iota((SUBS, LANES), 0)
    base = [jnp.zeros((SUBS, LANES), i32) for _ in wanted]
    for shift in range(21, -1, -3):
        tests = [b + ((subs + 1) << shift) for b in base]
        zero = jnp.zeros((SUBS, LANES), i32)

        def body(t, accs):
            accs = list(accs)
            for r in range(SUBS):
                one = jnp.broadcast_to(samples_ref[pl.ds(t * SUBS + r, 1), :], (SUBS, LANES))
                for n in range(len(tests)):
                    accs[n] = accs[n] + jnp.where(one < tests[n], 1, 0)
            return tuple(accs)

        accs = lax.fori_loop(0, LANES // SUBS, body, (zero,) * len(wanted))
        for n in range(len(wanted)):
            below = jnp.sum(accs[n].astype(f32), axis=1, keepdims=True)
            passed = jnp.where((below < wanted[n].astype(f32)) & (subs[:, :1] < SUBS - 1), 1, 0)
            digit = jnp.sum(passed, axis=0, keepdims=True)
            base[n] = base[n] + (jnp.broadcast_to(digit, (SUBS, LANES)) << shift)
    return base


def select(blocks_ref, samples_ref, turn_ref, in_ref):
    devices = blocks_ref.shape[0]
    d = lax.axis_index("gx") * lax.axis_size("gy") + lax.axis_index("gy")
    square = (LANES, LANES)
    samples_ref[...] = blocks_ref[:, SUBS - 1, :]
    wanted = [d * LANES, (d + 1) * LANES]
    low, high = splitter_key(samples_ref, wanted)
    high = jnp.where(d == devices - 1, BIG, high)
    samples = samples_ref[...]
    ends = [jnp.broadcast_to(k[:1, :], square) for k in (low, high)]
    ones = jnp.ones(square, bf16)
    below = jnp.where(iota(square, 1) < iota(square, 0), 1.0, 0.0).astype(bf16)

    def mm(a, b):
        return jnp.dot(a, b, preferred_element_type=f32)

    masks = []
    for k in ends:
        masks += [samples < k, samples <= k]
    counts = mm(jnp.concatenate([jnp.where(m, 1.0, 0.0).astype(bf16) for m in masks], axis=0), ones)
    counts = [counts[n * LANES : (n + 1) * LANES, :] for n in range(4)]
    taken, tied = [], []
    for n in range(2):
        lt, le = counts[2 * n], counts[2 * n + 1]
        equal = le - lt
        before = mm(below, equal.astype(bf16))
        total = mm(ones, lt.astype(bf16))
        left = jnp.asarray(wanted[n], f32) - total - before
        taken.append(lt + jnp.clip(left, 0.0, equal))
        tied.append(jnp.where(left > equal, 1, 0))
    first = taken[0]
    number = jnp.minimum(taken[1], LANES - 1.0) - first + 1.0
    start = mm(below, number.astype(bf16)).astype(i32)
    number, first, last = number.astype(i32), first.astype(i32), taken[1].astype(i32)
    lanes = iota(square, 1)
    turn_ref[...] = (lanes - (start - first)) & (LANES - 1)
    codes = []
    for h in range(2):
        m = lanes + h * LANES
        inside = (m >= start) & (m < start + number)
        in_ref[h] = jnp.where(inside, 1, 0)
        code = jnp.where(inside, 16, 0)
        code = code + jnp.where(inside & (m == start), 1 + tied[0], 0)
        code = code + jnp.where(inside & (m == start + last - first), 4 * (1 + tied[1]), 0)
        codes.append(code.astype(f32).astype(bf16))
    codes = mm(jnp.ones((SUBS, LANES), bf16), jnp.concatenate(codes, axis=1)).astype(i32)

    zero = jnp.zeros((SUBS, LANES), i32)

    def body(t, carry):
        carry = list(carry)
        for r in range(SUBS):
            b = t * SUBS + r
            turn = jnp.broadcast_to(turn_ref[pl.ds(b, 1), :], (SUBS, LANES))
            for c in range(2):
                tile = blocks_ref[b, c * SUBS : (c + 1) * SUBS, :]
                tile = jnp.take_along_axis(tile, turn, axis=1, mode="promise_in_bounds")
                for h in range(2):
                    inside = jnp.broadcast_to(in_ref[h, pl.ds(b, 1), :], (SUBS, LANES)) > 0
                    carry[2 * c + h] = jnp.where(inside, tile, carry[2 * c + h])
        return tuple(carry)

    k0, k1, v0, v1 = lax.fori_loop(0, devices // SUBS, body, (zero,) * 4)
    keys, valid = [], []
    for h, k in enumerate((k0, k1)):
        code = codes[:, h * LANES : (h + 1) * LANES]
        is_low, is_high = code & 3, (code >> 2) & 3
        ok = code >= 16
        ok = ok & ((is_low == 0) | (k >= low + is_low - 1))
        ok = ok & ((is_high == 0) | (k < high + is_high - 1))
        valid.append(jnp.where(ok, 1, 0))
        keys.append(jnp.where(ok, k, BIG))
    return keys, [v0, v1]


def place_kernel(found_ref, keys_out, values_out, size_out, digest_out):
    found = [found_ref[n * SUBS : (n + 1) * SUBS, :] for n in range(4)]
    keys, values = found[:2], found[2:]
    valid = jnp.where(keys[0] < BIG, 1, 0) + jnp.where(keys[1] < BIG, 1, 0)
    size = jnp.sum(jnp.sum(valid, axis=1, keepdims=True), axis=0, keepdims=True)
    ranks = candidate_ranks(keys)
    count = 2 * SUBS
    keys, values = placed(
        list(zip(keys, values)), [r >> 7 for r in ranks], [r & (LANES - 1) for r in ranks], count
    )
    rank = iota((count, LANES), 0) * LANES + iota((count, LANES), 1)
    filled = rank < size
    keys = jnp.where(filled, keys, -1)
    values = jnp.where(filled, values, -1)
    keys_out[...] = keys[: keys_out.shape[0], :]
    values_out[...] = values[: values_out.shape[0], :]
    mixed = (keys + 3 * values + 5 * rank) & 1023
    digest = jnp.where(filled, 2 * mixed - 1023, 0)
    digest = jnp.sum(jnp.sum(digest, axis=1, keepdims=True), axis=0, keepdims=True)
    size_out[0] = size[0, 0]
    digest_out[0] = digest[0, 0]


def candidates(keys, values, xs, planes):
    blocks = 2 * xs * planes
    dma = pltpu.SemaphoreType.DMA
    return pl.pallas_call(
        functools.partial(gather_kernel, xs, planes),
        out_shape=jax.ShapeDtypeStruct((4 * SUBS, LANES), i32),
        in_specs=[pl.BlockSpec(memory_space=pltpu.VMEM)] * 2,
        out_specs=pl.BlockSpec(memory_space=pltpu.VMEM),
        scratch_shapes=[
            pltpu.VMEM((2 * SUBS, LANES), i32),
            pltpu.VMEM((blocks, 2 * SUBS, LANES), i32),
            pltpu.VMEM((blocks, LANES), i32),
            pltpu.VMEM((blocks, LANES), i32),
            pltpu.VMEM((2, blocks, LANES), i32),
            dma,
            dma((xs,)),
            dma((xs,)),
            dma((xs,)),
        ],
        compiler_params=pltpu.CompilerParams(collective_id=0, has_side_effects=True),
        name="find_candidates",
    )(keys, values)


def placed_bucket(found, rows):
    one = jax.ShapeDtypeStruct((1,), i32)
    return pl.pallas_call(
        place_kernel,
        out_shape=(jax.ShapeDtypeStruct((rows, LANES), i32),) * 2 + (one, one),
        in_specs=[pl.BlockSpec(memory_space=pltpu.VMEM)],
        out_specs=[pl.BlockSpec(memory_space=pltpu.VMEM)] * 2 + [pl.BlockSpec(memory_space=pltpu.SMEM)] * 2,
        name="place_bucket",
    )(found)


def solution(mesh):
    gx, gy = mesh.shape["gx"], mesh.shape["gy"]

    def shards(record_keys, payloads):
        keys = record_keys.reshape(SUBS, LANES)
        values = payloads.reshape(SUBS, LANES)
        found = candidates(keys, values, gx // 2, gy)
        rows = (2 * record_keys.shape[0] - gx * gy) // LANES
        sorted_keys, sorted_values, size, digest = placed_bucket(found, rows)
        return sorted_keys.reshape(-1), sorted_values.reshape(-1), size, digest

    spec = P(("gx", "gy"))
    return jax.shard_map(shards, mesh=mesh, in_specs=(spec,) * 2, out_specs=(spec,) * 4, check_vma=False)
```

```python
import functools

import jax
import jax.numpy as jnp
from jax import lax
from jax.experimental import pallas as pl
from jax.experimental.pallas import tpu as pltpu
from jax.sharding import PartitionSpec as P

MESH = pl.DeviceIdType.MESH
LANES = 128
SUBS = 8
CHUNK = 256
CHUNKS = 3
BIG = 1 << 24
f32, bf16, i32 = jnp.float32, jnp.bfloat16, jnp.int32


def iota(shape, dim):
    return lax.broadcasted_iota(i32, shape, dim)


def row(x, s):
    return jnp.broadcast_to(x[s : s + 1, :], (SUBS, LANES))


def pieces(x):
    return [x & (CHUNK - 1), (x >> 8) & (CHUNK - 1), x >> 16]


def joined(parts):
    parts = [p.astype(i32) for p in parts]
    return parts[0] + (parts[1] << 8) + (parts[2] << 16)


def placed(rows, his, los, count):
    left, right = [], []
    for (keys, values), hi, lo in zip(rows, his, los):
        parts = [p.astype(f32) for p in pieces(keys) + pieces(values)]
        for s in range(SUBS):
            onehot = jnp.broadcast_to(lo[s : s + 1, :], (LANES, LANES)) == iota((LANES, LANES), 0)
            right.append(jnp.where(onehot, 1.0, 0.0).astype(bf16))
            column = []
            at = jnp.broadcast_to(hi[s : s + 1, :], (count, LANES)) == iota((count, LANES), 0)
            for p in parts:
                column.append(jnp.where(at, jnp.broadcast_to(p[s : s + 1, :], (count, LANES)), 0.0))
            left.append(jnp.concatenate(column, axis=0).astype(bf16))
    left = jnp.concatenate(left, axis=1)
    right = jnp.concatenate(right, axis=1)
    out = lax.dot_general(left, right, (((1,), (1,)), ((), ())), preferred_element_type=f32)
    out = [out[c * count : (c + 1) * count, :] for c in range(2 * CHUNKS)]
    return joined(out[:CHUNKS]), joined(out[CHUNKS:])


def sublane_sums(accs):
    return jnp.concatenate([jnp.sum(a, axis=0, keepdims=True) for a in accs], axis=0)


def column(x, m):
    return jnp.broadcast_to(x[:, m : m + 1], (SUBS, LANES))


def block_ranks(keys):
    subs, lanes = iota((SUBS, LANES), 0), iota((SUBS, LANES), 1)
    rows = [row(keys, s) + jnp.where(subs < s, 1, 0) for s in range(SUBS)]
    zero = jnp.zeros((SUBS, LANES), i32)
    accs, ties = [zero] * SUBS, zero
    for m in range(LANES):
        one = column(keys, m)
        for s in range(SUBS):
            accs[s] = accs[s] + jnp.where(one < rows[s], 1, 0)
        ties = ties + jnp.where((one == keys) & (lanes > m), 1, 0)
    return sublane_sums(accs) + ties


def candidate_ranks(halves):
    subs, lanes = iota((SUBS, LANES), 0), iota((SUBS, LANES), 1)
    zero = jnp.zeros((SUBS, LANES), i32)
    ranks = []
    for target, keys in enumerate(halves):
        rows = [row(keys, s) for s in range(SUBS)]
        accs = [zero] * SUBS
        for source, others in enumerate(halves):
            if target > source:
                others = others - 1
            for m in range(LANES):
                one = column(others, m)
                if target == source:
                    one = one - jnp.where(lanes > m, 1, 0)
                for s in range(SUBS):
                    accs[s] = accs[s] + jnp.where(one < rows[s], 1, 0)
        ties = zero
        for d in range(1, SUBS):
            ties = ties + jnp.where((pltpu.roll(keys, d, 0) == keys) & (subs >= d), 1, 0)
        ranks.append(sublane_sums(accs) + ties)
    return ranks


def sorted_block(keys, values):
    rank = block_ranks(keys)
    return placed([(keys, values)], [rank & (SUBS - 1)], [rank >> 3], SUBS)


HALF = SUBS // 2
TALL = SUBS + HALF
SHIFT = BIG // 2
AXIS = 4


def hops(offset):
    return sum(min(k, AXIS - k) for k in offset)


OFFSETS = sorted(((dx, dz, dy) for dx in range(AXIS) for dz in range(AXIS) for dy in range(AXIS)), key=lambda o: -hops(o))


def gather_kernel(
    keys_ref,
    values_ref,
    found_ref,
    sample,
    block,
    rows,
    blocks,
    turns,
    inside,
    row_send,
    row_recv,
    send_sem,
    recv_sem,
    give_sem,
    take_sem,
):
    gx, gy = lax.axis_index("gx"), lax.axis_index("gy")
    x, core, z, y = gx // 2, gx % 2, gy // AXIS, gy % AXIS
    planes = AXIS * AXIS
    devices = 2 * AXIS * planes
    me = gx * planes + gy
    barrier = pltpu.get_barrier_semaphore()

    def device(offset, other):
        dx, dz, dy = offset
        which = 1 - core if other else core
        return ((x + dx) % AXIS) * 2 + which, ((z + dz) % AXIS) * AXIS + (y + dy) % AXIS

    peers = [(o, device(o, other), other) for o in OFFSETS for other in (1, 0) if other or hops(o)]
    for _, peer, _ in peers:
        pl.semaphore_signal(barrier, inc=1, device_id=peer, device_id_type=MESH)

    keys, values = sorted_block(keys_ref[...], values_ref[...])
    for ref in (sample, rows.at[me]):
        ref[...] = keys[SUBS - 1 :, :]
    for ref in (block, blocks.at[me]):
        ref[:SUBS, :] = ((keys - SHIFT) << 8) | (values >> 16)
        ref[SUBS:, :] = (values[:HALF, :] & 0xFFFF) | (values[HALF:, :] << 16)
    pl.semaphore_wait(barrier, devices - 1)

    for _, peer, _ in peers:
        pltpu.make_async_remote_copy(
            src_ref=sample,
            dst_ref=rows.at[me],
            send_sem=row_send,
            recv_sem=row_recv,
            device_id=peer,
            device_id_type=MESH,
        ).start()
    for (dx, dz, dy), peer, other in peers:
        if not other:
            pltpu.make_async_remote_copy(
                src_ref=block,
                dst_ref=blocks.at[me],
                send_sem=send_sem,
                recv_sem=recv_sem.at[(AXIS - dx) % AXIS],
                device_id=peer,
                device_id_type=MESH,
            ).start()

    all_rows = rows.at[pl.ds(0, devices - 1)]
    pltpu.make_async_copy(all_rows, all_rows, row_recv).wait()
    wanted = [me * LANES, (me + 1) * LANES]
    found = [jnp.zeros((SUBS, LANES), i32)] * 2
    found = search(rows, wanted, found, SHIFTS[:EARLY])
    gives = []
    for dx in (0, 1, 3, 2):
        at = (((x + dx) % AXIS) * 2 + core) * planes
        arrived = blocks.at[pl.ds(at, planes if dx else planes - 1)]
        pltpu.make_async_copy(arrived, arrived, recv_sem.at[dx]).wait()
        group = blocks.at[pl.ds(at, planes)]
        give = pltpu.make_async_remote_copy(
            src_ref=group,
            dst_ref=group,
            send_sem=give_sem.at[dx],
            recv_sem=take_sem.at[dx],
            device_id=(x * 2 + 1 - core, gy),
            device_id_type=MESH,
        )
        give.start()
        gives.append(give)
    low, high = search(rows, wanted, found, SHIFTS[EARLY:])
    high = jnp.where(me == devices - 1, BIG, high)
    codes = group_plan(wanted, low, high, rows, turns, inside)
    tiles = [jnp.zeros((SUBS, LANES), i32)] * 4
    tiles = collect(tiles, blocks, turns, inside, core)
    for give in gives:
        give.wait_recv()
    tiles = collect(tiles, blocks, turns, inside, 1 - core)
    keys, values = unpacked(tiles, codes, low, high)
    for n, tile in enumerate(keys + values):
        found_ref[n * SUBS : (n + 1) * SUBS, :] = tile
    pltpu.make_async_copy(all_rows, all_rows, row_send).wait()
    sent = blocks.at[pl.ds(0, AXIS * planes - 1)]
    pltpu.make_async_copy(sent, sent, send_sem).wait()
    for give in gives:
        give.wait_send()


SHIFTS = tuple(range(21, -1, -3))
EARLY = 4


def search(rows_ref, wanted, base, shifts):
    subs = iota((SUBS, LANES), 0)
    base = list(base)
    zero = jnp.zeros((SUBS, LANES), i32)
    for shift in shifts:
        tests = [b + ((subs + 1) << shift) for b in base]
        accs = [[zero, zero] for _ in tests]
        for r in range(LANES):
            one = jnp.broadcast_to(rows_ref[r], (SUBS, LANES))
            for n, test in enumerate(tests):
                accs[n][r % 2] = accs[n][r % 2] + jnp.where(one < test, 1, 0)
        for n in range(len(wanted)):
            below = jnp.sum((accs[n][0] + accs[n][1]).astype(f32), axis=1, keepdims=True)
            passed = jnp.where((below < wanted[n].astype(f32)) & (subs[:, :1] < SUBS - 1), 1, 0)
            digit = jnp.sum(passed, axis=0, keepdims=True)
            base[n] = base[n] + (jnp.broadcast_to(digit, (SUBS, LANES)) << shift)
    return base


def group_plan(wanted, low, high, rows_ref, turn_ref, in_ref):
    square = (LANES, LANES)
    samples = rows_ref[...].reshape(square)
    ends = [jnp.broadcast_to(k[:1, :], square) for k in (low, high)]
    ones = jnp.ones(square, bf16)
    below = jnp.where(iota(square, 1) < iota(square, 0), 1.0, 0.0).astype(bf16)

    def mm(a, b):
        return jnp.dot(a, b, preferred_element_type=f32)

    masks = []
    for k in ends:
        masks += [samples < k, samples <= k]
    counts = mm(jnp.concatenate([jnp.where(m, 1.0, 0.0).astype(bf16) for m in masks], axis=0), ones)
    counts = [counts[n * LANES : (n + 1) * LANES, :] for n in range(4)]
    taken, tied = [], []
    for n in range(2):
        lt, le = counts[2 * n], counts[2 * n + 1]
        equal = le - lt
        before = mm(below, equal.astype(bf16))
        total = mm(ones, lt.astype(bf16))
        left = jnp.asarray(wanted[n], f32) - total - before
        taken.append(lt + jnp.clip(left, 0.0, equal))
        tied.append(jnp.where(left > equal, 1, 0))
    first = taken[0]
    number = jnp.minimum(taken[1], LANES - 1.0) - first + 1.0
    start = mm(below, number.astype(bf16)).astype(i32)
    number, first, last = number.astype(i32), first.astype(i32), taken[1].astype(i32)
    lanes = iota(square, 1)
    turn_ref[...] = (lanes - (start - first)) & (LANES - 1)
    codes = []
    for h in range(2):
        m = lanes + h * LANES
        inside = (m >= start) & (m < start + number)
        in_ref[h] = jnp.where(inside, 1, 0)
        code = jnp.where(inside, 16, 0)
        code = code + jnp.where(inside & (m == start), 1 + tied[0], 0)
        code = code + jnp.where(inside & (m == start + last - first), 4 * (1 + tied[1]), 0)
        codes.append(code.astype(f32).astype(bf16))
    return mm(jnp.ones((SUBS, LANES), bf16), jnp.concatenate(codes, axis=1)).astype(i32)


def collect(tiles, blocks_ref, turn_ref, in_ref, core):
    tiles = list(tiles)
    planes = AXIS * AXIS
    for at in range(AXIS * planes):
        b = (at // planes * 2 + core) * planes + at % planes
        turn = jnp.broadcast_to(turn_ref[pl.ds(b, 1), :], (SUBS, LANES))
        rest = blocks_ref[b, SUBS:, :]
        for c, tile in enumerate((blocks_ref[b, :SUBS, :], jnp.concatenate([rest, rest], axis=0))):
            tile = jnp.take_along_axis(tile, turn, axis=1, mode="promise_in_bounds")
            for h in range(2):
                inside = jnp.broadcast_to(in_ref[h, pl.ds(b, 1), :], (SUBS, LANES)) > 0
                tiles[2 * c + h] = jnp.where(inside, tile, tiles[2 * c + h])
    return tiles


def unpacked(tiles, codes, low, high):
    upper = iota((SUBS, LANES), 0) >= HALF
    keys, values = [], []
    for h in range(2):
        w, r = tiles[h], tiles[2 + h]
        k = (w >> 8) + SHIFT
        values.append(((w & 255) << 16) | (jnp.where(upper, r >> 16, r) & 0xFFFF))
        code = codes[:, h * LANES : (h + 1) * LANES]
        is_low, is_high = code & 3, (code >> 2) & 3
        ok = code >= 16
        ok = ok & ((is_low == 0) | (k >= low + is_low - 1))
        ok = ok & ((is_high == 0) | (k < high + is_high - 1))
        keys.append(jnp.where(ok, k, BIG))
    return keys, values


def place_kernel(found_ref, keys_out, values_out, size_out, digest_out):
    found = [found_ref[n * SUBS : (n + 1) * SUBS, :] for n in range(4)]
    keys, values = found[:2], found[2:]
    valid = jnp.where(keys[0] < BIG, 1, 0) + jnp.where(keys[1] < BIG, 1, 0)
    size = jnp.sum(jnp.sum(valid, axis=1, keepdims=True), axis=0, keepdims=True)
    ranks = candidate_ranks(keys)
    count = 2 * SUBS
    keys, values = placed(
        list(zip(keys, values)), [r >> 7 for r in ranks], [r & (LANES - 1) for r in ranks], count
    )
    rank = iota((count, LANES), 0) * LANES + iota((count, LANES), 1)
    filled = rank < size
    keys = jnp.where(filled, keys, -1)
    values = jnp.where(filled, values, -1)
    keys_out[...] = keys[: keys_out.shape[0], :]
    values_out[...] = values[: values_out.shape[0], :]
    mixed = (keys + 3 * values + 5 * rank) & 1023
    digest = jnp.where(filled, 2 * mixed - 1023, 0)
    digest = jnp.sum(jnp.sum(digest, axis=1, keepdims=True), axis=0, keepdims=True)
    size_out[0] = size[0, 0]
    digest_out[0] = digest[0, 0]


def candidates(keys, values):
    dma = pltpu.SemaphoreType.DMA
    return pl.pallas_call(
        gather_kernel,
        out_shape=jax.ShapeDtypeStruct((4 * SUBS, LANES), i32),
        in_specs=[pl.BlockSpec(memory_space=pltpu.VMEM)] * 2,
        out_specs=pl.BlockSpec(memory_space=pltpu.VMEM),
        scratch_shapes=[
            pltpu.VMEM((1, LANES), i32),
            pltpu.VMEM((TALL, LANES), i32),
            pltpu.VMEM((LANES, 1, LANES), i32),
            pltpu.VMEM((LANES, TALL, LANES), i32),
            pltpu.VMEM((LANES, LANES), i32),
            pltpu.VMEM((2, LANES, LANES), i32),
            dma,
            dma,
            dma,
            dma((AXIS,)),
            dma((AXIS,)),
            dma((AXIS,)),
        ],
        compiler_params=pltpu.CompilerParams(collective_id=0, has_side_effects=True),
        name="find_candidates",
    )(keys, values)


def placed_bucket(found, rows):
    one = jax.ShapeDtypeStruct((1,), i32)
    return pl.pallas_call(
        place_kernel,
        out_shape=(jax.ShapeDtypeStruct((rows, LANES), i32),) * 2 + (one, one),
        in_specs=[pl.BlockSpec(memory_space=pltpu.VMEM)],
        out_specs=[pl.BlockSpec(memory_space=pltpu.VMEM)] * 2 + [pl.BlockSpec(memory_space=pltpu.SMEM)] * 2,
        name="place_bucket",
    )(found)


def solution(mesh):
    gx, gy = mesh.shape["gx"], mesh.shape["gy"]

    def shards(record_keys, payloads):
        keys = record_keys.reshape(SUBS, LANES)
        values = payloads.reshape(SUBS, LANES)
        found = candidates(keys, values)
        rows = (2 * record_keys.shape[0] - gx * gy) // LANES
        sorted_keys, sorted_values, size, digest = placed_bucket(found, rows)
        return sorted_keys.reshape(-1), sorted_values.reshape(-1), size, digest

    spec = P(("gx", "gy"))
    return jax.shard_map(shards, mesh=mesh, in_specs=(spec,) * 2, out_specs=(spec,) * 4, check_vma=False)
```

```python
import functools

import jax
import jax.numpy as jnp
from jax import lax
from jax.experimental import pallas as pl
from jax.experimental.pallas import tpu as pltpu
from jax.sharding import PartitionSpec as P

MESH = pl.DeviceIdType.MESH
LANES = 128
SUBS = 8
CHUNK = 256
CHUNKS = 3
BIG = 1 << 24
f32, bf16, i32 = jnp.float32, jnp.bfloat16, jnp.int32


def iota(shape, dim):
    return lax.broadcasted_iota(i32, shape, dim)


def row(x, s):
    return jnp.broadcast_to(x[s : s + 1, :], (SUBS, LANES))


def pieces(x):
    return [x & (CHUNK - 1), (x >> 8) & (CHUNK - 1), x >> 16]


def joined(parts):
    parts = [p.astype(i32) for p in parts]
    return parts[0] + (parts[1] << 8) + (parts[2] << 16)


def placed(rows, his, los, count):
    left, right = [], []
    for (keys, values), hi, lo in zip(rows, his, los):
        parts = [p.astype(f32) for p in pieces(keys) + pieces(values)]
        for s in range(SUBS):
            onehot = jnp.broadcast_to(lo[s : s + 1, :], (LANES, LANES)) == iota((LANES, LANES), 0)
            right.append(jnp.where(onehot, 1.0, 0.0).astype(bf16))
            column = []
            at = jnp.broadcast_to(hi[s : s + 1, :], (count, LANES)) == iota((count, LANES), 0)
            for p in parts:
                column.append(jnp.where(at, jnp.broadcast_to(p[s : s + 1, :], (count, LANES)), 0.0))
            left.append(jnp.concatenate(column, axis=0).astype(bf16))
    left = jnp.concatenate(left, axis=1)
    right = jnp.concatenate(right, axis=1)
    out = lax.dot_general(left, right, (((1,), (1,)), ((), ())), preferred_element_type=f32)
    out = [out[c * count : (c + 1) * count, :] for c in range(2 * CHUNKS)]
    return joined(out[:CHUNKS]), joined(out[CHUNKS:])


def sublane_sums(accs):
    return jnp.concatenate([jnp.sum(a, axis=0, keepdims=True) for a in accs], axis=0)


def column(x, m):
    return jnp.broadcast_to(x[:, m : m + 1], (SUBS, LANES))


def block_ranks(keys):
    subs, lanes = iota((SUBS, LANES), 0), iota((SUBS, LANES), 1)
    rows = [row(keys, s) + jnp.where(subs < s, 1, 0) for s in range(SUBS)]
    zero = jnp.zeros((SUBS, LANES), i32)
    accs, ties = [zero] * SUBS, zero
    for m in range(LANES):
        one = column(keys, m)
        for s in range(SUBS):
            accs[s] = accs[s] + jnp.where(one < rows[s], 1, 0)
        ties = ties + jnp.where((one == keys) & (lanes > m), 1, 0)
    return sublane_sums(accs) + ties


def candidate_ranks(halves):
    subs, lanes = iota((SUBS, LANES), 0), iota((SUBS, LANES), 1)
    zero = jnp.zeros((SUBS, LANES), i32)
    ranks = []
    for target, keys in enumerate(halves):
        rows = [row(keys, s) for s in range(SUBS)]
        accs = [zero] * SUBS
        for source, others in enumerate(halves):
            if target > source:
                others = others - 1
            for m in range(LANES):
                one = column(others, m)
                if target == source:
                    one = one - jnp.where(lanes > m, 1, 0)
                for s in range(SUBS):
                    accs[s] = accs[s] + jnp.where(one < rows[s], 1, 0)
        ties = zero
        for d in range(1, SUBS):
            ties = ties + jnp.where((pltpu.roll(keys, d, 0) == keys) & (subs >= d), 1, 0)
        ranks.append(sublane_sums(accs) + ties)
    return ranks


def sorted_block(keys, values):
    rank = block_ranks(keys)
    return placed([(keys, values)], [rank & (SUBS - 1)], [rank >> 3], SUBS)


SHORT = 6
BYTE = 24
AXIS = 4


def packed(x):
    extra = [(x[SHORT + r // 3 : SHORT + r // 3 + 1, :] >> (8 * (r % 3))) & 255 for r in range(SHORT)]
    return x[:SHORT, :] | (jnp.concatenate(extra, axis=0) << BYTE)


def unpacked(x):
    extra = (x >> BYTE) & 255
    last = [extra[r : r + 1, :] | (extra[r + 1 : r + 2, :] << 8) | (extra[r + 2 : r + 3, :] << 16) for r in (0, 3)]
    return jnp.concatenate([x[:SHORT, :] & (BIG - 1)] + last, axis=0)


def hops(offset):
    return sum(min(k, AXIS - k) for k in offset)


OFFSETS = sorted(((dx, dz, dy) for dx in range(AXIS) for dz in range(AXIS) for dy in range(AXIS)), key=lambda o: -hops(o))


def gather_kernel(
    keys_hbm,
    values_hbm,
    found_ref,
    local,
    sample,
    block,
    rows,
    blocks,
    turns,
    inside,
    local_sem,
    row_send,
    row_recv,
    send_sem,
    recv_sem,
    give_sem,
    take_sem,
):
    gx, gy = lax.axis_index("gx"), lax.axis_index("gy")
    x, core, z, y = gx // 2, gx % 2, gy // AXIS, gy % AXIS
    planes = AXIS * AXIS
    devices = 2 * AXIS * planes
    me = gx * planes + gy
    barrier = pltpu.get_barrier_semaphore()
    loads = [pltpu.make_async_copy(ref, local.at[c], local_sem.at[c]) for c, ref in enumerate((keys_hbm, values_hbm))]
    for load in loads:
        load.start()

    def device(offset, other):
        dx, dz, dy = offset
        which = 1 - core if other else core
        return ((x + dx) % AXIS) * 2 + which, ((z + dz) % AXIS) * AXIS + (y + dy) % AXIS

    peers = [(o, device(o, other), other) for o in OFFSETS for other in (1, 0) if other or hops(o)]
    for _, peer, _ in peers:
        pl.semaphore_signal(barrier, inc=1, device_id=peer, device_id_type=MESH)
    for load in loads:
        load.wait()

    keys, values = sorted_block(local[0], local[1])
    for ref in (sample, rows.at[me]):
        ref[...] = keys[SUBS - 1 :, :]
    for c, tile in enumerate((keys, values)):
        tile = packed(tile)
        block[c] = tile
        blocks[c, me] = tile
    pl.semaphore_wait(barrier, devices - 1)

    for _, peer, _ in peers:
        pltpu.make_async_remote_copy(
            src_ref=sample,
            dst_ref=rows.at[me],
            send_sem=row_send,
            recv_sem=row_recv,
            device_id=peer,
            device_id_type=MESH,
        ).start()
    for c in range(2):
        for (dx, dz, dy), peer, other in peers:
            if not other:
                pltpu.make_async_remote_copy(
                    src_ref=block.at[c],
                    dst_ref=blocks.at[c, me],
                    send_sem=send_sem.at[c],
                    recv_sem=recv_sem.at[c, (AXIS - dx) % AXIS],
                    device_id=peer,
                    device_id_type=MESH,
                ).start()

    def forward(c):
        gives = []
        for dx in (0, 1, 3, 2):
            at = (((x + dx) % AXIS) * 2 + core) * planes
            arrived = blocks.at[c, pl.ds(at, planes if dx else planes - 1)]
            pltpu.make_async_copy(arrived, arrived, recv_sem.at[c, dx]).wait()
            group = blocks.at[c, pl.ds(at, planes)]
            give = pltpu.make_async_remote_copy(
                src_ref=group,
                dst_ref=group,
                send_sem=give_sem.at[c, dx],
                recv_sem=take_sem.at[c, dx],
                device_id=(x * 2 + 1 - core, gy),
                device_id_type=MESH,
            )
            give.start()
            gives.append(give)
        return gives

    all_rows = rows.at[pl.ds(0, devices - 1)]
    pltpu.make_async_copy(all_rows, all_rows, row_recv).wait()
    wanted = [me * LANES, (me + 1) * LANES]
    zero = jnp.zeros((SUBS, LANES), i32)
    ends = search(rows, wanted, [zero] * 2, SHIFTS[:EARLY])
    key_gives = forward(0)
    low, high = search(rows, wanted, ends, SHIFTS[EARLY:])
    high = jnp.where(me == devices - 1, BIG, high)
    codes = group_plan(wanted, low, high, rows, turns, inside)
    tiles = collect([zero] * 2, blocks, 0, turns, inside, core)
    value_gives = forward(1)
    for give in key_gives:
        give.wait_recv()
    tiles = collect(tiles, blocks, 0, turns, inside, 1 - core)
    keys = bucket_keys(tiles, codes, low, high)
    ranks = candidate_ranks(keys)
    tiles = collect([zero] * 2, blocks, 1, turns, inside, core)
    for give in value_gives:
        give.wait_recv()
    tiles = collect(tiles, blocks, 1, turns, inside, 1 - core)
    for n, tile in enumerate(keys + [unpacked(t) for t in tiles] + ranks):
        found_ref[n * SUBS : (n + 1) * SUBS, :] = tile
    pltpu.make_async_copy(all_rows, all_rows, row_send).wait()
    for c in range(2):
        sent = blocks.at[c, pl.ds(0, AXIS * planes - 1)]
        pltpu.make_async_copy(sent, sent, send_sem.at[c]).wait()
    for give in key_gives + value_gives:
        give.wait_send()


SHIFTS = tuple(range(21, -1, -3))
EARLY = 4


def search(rows_ref, wanted, base, shifts):
    subs = iota((SUBS, LANES), 0)
    base = list(base)
    zero = jnp.zeros((SUBS, LANES), i32)
    for shift in shifts:
        tests = [b + ((subs + 1) << shift) for b in base]
        accs = [[zero, zero] for _ in tests]
        for r in range(LANES):
            one = jnp.broadcast_to(rows_ref[r], (SUBS, LANES))
            for n, test in enumerate(tests):
                accs[n][r % 2] = accs[n][r % 2] + jnp.where(one < test, 1, 0)
        for n in range(len(wanted)):
            below = jnp.sum((accs[n][0] + accs[n][1]).astype(f32), axis=1, keepdims=True)
            passed = jnp.where((below < wanted[n].astype(f32)) & (subs[:, :1] < SUBS - 1), 1, 0)
            digit = jnp.sum(passed, axis=0, keepdims=True)
            base[n] = base[n] + (jnp.broadcast_to(digit, (SUBS, LANES)) << shift)
    return base


def group_plan(wanted, low, high, rows_ref, turn_ref, in_ref):
    square = (LANES, LANES)
    samples = rows_ref[...].reshape(square)
    ends = [jnp.broadcast_to(k[:1, :], square) for k in (low, high)]
    ones = jnp.ones(square, bf16)
    below = jnp.where(iota(square, 1) < iota(square, 0), 1.0, 0.0).astype(bf16)

    def mm(a, b):
        return jnp.dot(a, b, preferred_element_type=f32)

    masks = []
    for k in ends:
        masks += [samples < k, samples <= k]
    counts = mm(jnp.concatenate([jnp.where(m, 1.0, 0.0).astype(bf16) for m in masks], axis=0), ones)
    counts = [counts[n * LANES : (n + 1) * LANES, :] for n in range(4)]
    taken, tied = [], []
    for n in range(2):
        lt, le = counts[2 * n], counts[2 * n + 1]
        equal = le - lt
        before = mm(below, equal.astype(bf16))
        total = mm(ones, lt.astype(bf16))
        left = jnp.asarray(wanted[n], f32) - total - before
        taken.append(lt + jnp.clip(left, 0.0, equal))
        tied.append(jnp.where(left > equal, 1, 0))
    first = taken[0]
    number = jnp.minimum(taken[1], LANES - 1.0) - first + 1.0
    start = mm(below, number.astype(bf16)).astype(i32)
    number, first, last = number.astype(i32), first.astype(i32), taken[1].astype(i32)
    lanes = iota(square, 1)
    turn_ref[...] = (lanes - (start - first)) & (LANES - 1)
    codes = []
    for h in range(2):
        m = lanes + h * LANES
        inside = (m >= start) & (m < start + number)
        in_ref[h] = jnp.where(inside, 1, 0)
        code = jnp.where(inside, 16, 0)
        code = code + jnp.where(inside & (m == start), 1 + tied[0], 0)
        code = code + jnp.where(inside & (m == start + last - first), 4 * (1 + tied[1]), 0)
        codes.append(code.astype(f32).astype(bf16))
    return mm(jnp.ones((SUBS, LANES), bf16), jnp.concatenate(codes, axis=1)).astype(i32)


def collect(tiles, blocks_ref, c, turn_ref, in_ref, core):
    tiles = list(tiles)
    planes = AXIS * AXIS
    empty = jnp.zeros((SUBS - SHORT, LANES), i32)
    for at in range(AXIS * planes):
        b = (at // planes * 2 + core) * planes + at % planes
        turn = jnp.broadcast_to(turn_ref[pl.ds(b, 1), :], (SUBS, LANES))
        tile = jnp.concatenate([blocks_ref[c, b], empty], axis=0)
        tile = jnp.take_along_axis(tile, turn, axis=1, mode="promise_in_bounds")
        for h in range(2):
            here = jnp.broadcast_to(in_ref[h, pl.ds(b, 1), :], (SUBS, LANES)) > 0
            tiles[h] = jnp.where(here, tile, tiles[h])
    return tiles


def bucket_keys(tiles, codes, low, high):
    keys = []
    for h, tile in enumerate(tiles):
        k = unpacked(tile)
        code = codes[:, h * LANES : (h + 1) * LANES]
        is_low, is_high = code & 3, (code >> 2) & 3
        ok = code >= 16
        ok = ok & ((is_low == 0) | (k >= low + is_low - 1))
        ok = ok & ((is_high == 0) | (k < high + is_high - 1))
        keys.append(jnp.where(ok, k, BIG))
    return keys


def place_kernel(found_ref, keys_out, values_out, size_out, digest_out):
    found = [found_ref[n * SUBS : (n + 1) * SUBS, :] for n in range(6)]
    keys, values, ranks = found[:2], found[2:4], found[4:]
    valid = jnp.where(keys[0] < BIG, 1, 0) + jnp.where(keys[1] < BIG, 1, 0)
    size = jnp.sum(jnp.sum(valid, axis=1, keepdims=True), axis=0, keepdims=True)
    count = 2 * SUBS
    keys, values = placed(
        list(zip(keys, values)), [r >> 7 for r in ranks], [r & (LANES - 1) for r in ranks], count
    )
    rank = iota((count, LANES), 0) * LANES + iota((count, LANES), 1)
    filled = rank < size
    keys = jnp.where(filled, keys, -1)
    values = jnp.where(filled, values, -1)
    keys_out[...] = keys[: keys_out.shape[0], :]
    values_out[...] = values[: values_out.shape[0], :]
    mixed = (keys + 3 * values + 5 * rank) & 1023
    digest = jnp.where(filled, 2 * mixed - 1023, 0)
    digest = jnp.sum(jnp.sum(digest, axis=1, keepdims=True), axis=0, keepdims=True)
    size_out[0] = size[0, 0]
    digest_out[0] = digest[0, 0]


def candidates(keys, values):
    dma = pltpu.SemaphoreType.DMA
    return pl.pallas_call(
        gather_kernel,
        out_shape=jax.ShapeDtypeStruct((6 * SUBS, LANES), i32),
        in_specs=[pl.BlockSpec(memory_space=pltpu.HBM)] * 2,
        out_specs=pl.BlockSpec(memory_space=pltpu.VMEM),
        scratch_shapes=[
            pltpu.VMEM((2, SUBS, LANES), i32),
            pltpu.VMEM((1, LANES), i32),
            pltpu.VMEM((2, SHORT, LANES), i32),
            pltpu.VMEM((LANES, 1, LANES), i32),
            pltpu.VMEM((2, LANES, SHORT, LANES), i32),
            pltpu.VMEM((LANES, LANES), i32),
            pltpu.VMEM((2, LANES, LANES), i32),
            dma((2,)),
            dma,
            dma,
            dma((2,)),
            dma((2, AXIS)),
            dma((2, AXIS)),
            dma((2, AXIS)),
        ],
        compiler_params=pltpu.CompilerParams(collective_id=0, has_side_effects=True),
        name="find_candidates",
    )(keys, values)


def placed_bucket(found, rows):
    one = jax.ShapeDtypeStruct((1,), i32)
    return pl.pallas_call(
        place_kernel,
        out_shape=(jax.ShapeDtypeStruct((rows, LANES), i32),) * 2 + (one, one),
        in_specs=[pl.BlockSpec(memory_space=pltpu.VMEM)],
        out_specs=[pl.BlockSpec(memory_space=pltpu.VMEM)] * 2 + [pl.BlockSpec(memory_space=pltpu.SMEM)] * 2,
        name="place_bucket",
    )(found)


def solution(mesh):
    gx, gy = mesh.shape["gx"], mesh.shape["gy"]

    def shards(record_keys, payloads):
        keys = record_keys.reshape(SUBS, LANES)
        values = payloads.reshape(SUBS, LANES)
        found = candidates(keys, values)
        rows = (2 * record_keys.shape[0] - gx * gy) // LANES
        sorted_keys, sorted_values, size, digest = placed_bucket(found, rows)
        return sorted_keys.reshape(-1), sorted_values.reshape(-1), size, digest

    spec = P(("gx", "gy"))
    return jax.shard_map(shards, mesh=mesh, in_specs=(spec,) * 2, out_specs=(spec,) * 4, check_vma=False)
```

```python
import functools

import jax
import jax.numpy as jnp
from jax import lax
from jax.experimental import pallas as pl
from jax.experimental.pallas import tpu as pltpu
from jax.sharding import PartitionSpec as P

MESH = pl.DeviceIdType.MESH
LANES = 128
SUBS = 8
CHUNK = 256
CHUNKS = 3
BIG = 1 << 24
f32, bf16, i32 = jnp.float32, jnp.bfloat16, jnp.int32


def iota(shape, dim):
    return lax.broadcasted_iota(i32, shape, dim)


def row(x, s):
    return jnp.broadcast_to(x[s : s + 1, :], (SUBS, LANES))


def pieces(x):
    return [x & (CHUNK - 1), (x >> 8) & (CHUNK - 1), x >> 16]


def joined(parts):
    parts = [p.astype(i32) for p in parts]
    return parts[0] + (parts[1] << 8) + (parts[2] << 16)


def placed(rows, his, los, count):
    left, right = [], []
    for (keys, values), hi, lo in zip(rows, his, los):
        parts = [p.astype(f32) for p in pieces(keys) + pieces(values)]
        for s in range(SUBS):
            onehot = jnp.broadcast_to(lo[s : s + 1, :], (LANES, LANES)) == iota((LANES, LANES), 0)
            right.append(jnp.where(onehot, 1.0, 0.0).astype(bf16))
            column = []
            at = jnp.broadcast_to(hi[s : s + 1, :], (count, LANES)) == iota((count, LANES), 0)
            for p in parts:
                column.append(jnp.where(at, jnp.broadcast_to(p[s : s + 1, :], (count, LANES)), 0.0))
            left.append(jnp.concatenate(column, axis=0).astype(bf16))
    left = jnp.concatenate(left, axis=1)
    right = jnp.concatenate(right, axis=1)
    out = lax.dot_general(left, right, (((1,), (1,)), ((), ())), preferred_element_type=f32)
    out = [out[c * count : (c + 1) * count, :] for c in range(2 * CHUNKS)]
    return joined(out[:CHUNKS]), joined(out[CHUNKS:])


def sublane_sums(accs):
    return jnp.concatenate([jnp.sum(a, axis=0, keepdims=True) for a in accs], axis=0)


def column(x, m):
    return jnp.broadcast_to(x[:, m : m + 1], (SUBS, LANES))


def block_ranks(keys):
    subs, lanes = iota((SUBS, LANES), 0), iota((SUBS, LANES), 1)
    rows = [row(keys, s) + jnp.where(subs < s, 1, 0) for s in range(SUBS)]
    zero = jnp.zeros((SUBS, LANES), i32)
    accs, ties = [zero] * SUBS, zero
    for m in range(LANES):
        one = column(keys, m)
        for s in range(SUBS):
            accs[s] = accs[s] + jnp.where(one < rows[s], 1, 0)
        ties = ties + jnp.where((one == keys) & (lanes > m), 1, 0)
    return sublane_sums(accs) + ties


def candidate_ranks(halves):
    subs, lanes = iota((SUBS, LANES), 0), iota((SUBS, LANES), 1)
    zero = jnp.zeros((SUBS, LANES), i32)
    ranks = []
    for target, keys in enumerate(halves):
        rows = [row(keys, s) for s in range(SUBS)]
        accs = [zero] * SUBS
        for source, others in enumerate(halves):
            if target > source:
                others = others - 1
            for m in range(LANES):
                one = column(others, m)
                if target == source:
                    one = one - jnp.where(lanes > m, 1, 0)
                for s in range(SUBS):
                    accs[s] = accs[s] + jnp.where(one < rows[s], 1, 0)
        ties = zero
        for d in range(1, SUBS):
            ties = ties + jnp.where((pltpu.roll(keys, d, 0) == keys) & (subs >= d), 1, 0)
        ranks.append(sublane_sums(accs) + ties)
    return ranks


def sorted_block(keys, values):
    rank = block_ranks(keys)
    return placed([(keys, values)], [rank & (SUBS - 1)], [rank >> 3], SUBS)


SHORT = 6
BYTE = 24
AXIS = 4


def packed(x):
    extra = [(x[SHORT + r // 3 : SHORT + r // 3 + 1, :] >> (8 * (r % 3))) & 255 for r in range(SHORT)]
    return x[:SHORT, :] | (jnp.concatenate(extra, axis=0) << BYTE)


def unpacked(x):
    extra = (x >> BYTE) & 255
    last = [extra[r : r + 1, :] | (extra[r + 1 : r + 2, :] << 8) | (extra[r + 2 : r + 3, :] << 16) for r in (0, 3)]
    return jnp.concatenate([x[:SHORT, :] & (BIG - 1)] + last, axis=0)


def hops(offset):
    return sum(min(k, AXIS - k) for k in offset)


OFFSETS = sorted(((dx, dz, dy) for dx in range(AXIS) for dz in range(AXIS) for dy in range(AXIS)), key=lambda o: -hops(o))


def gather_kernel(
    keys_hbm,
    values_hbm,
    found_ref,
    local,
    sample,
    block,
    rows,
    blocks,
    turns,
    inside,
    local_sem,
    row_send,
    row_recv,
    send_sem,
    recv_sem,
    give_sem,
    take_sem,
):
    gx, gy = lax.axis_index("gx"), lax.axis_index("gy")
    x, core, z, y = gx // 2, gx % 2, gy // AXIS, gy % AXIS
    planes = AXIS * AXIS
    devices = 2 * AXIS * planes
    me = gx * planes + gy
    barrier = pltpu.get_barrier_semaphore()
    loads = [pltpu.make_async_copy(ref, local.at[c], local_sem.at[c]) for c, ref in enumerate((keys_hbm, values_hbm))]
    for load in loads:
        load.start()

    def device(offset, other):
        dx, dz, dy = offset
        which = 1 - core if other else core
        return ((x + dx) % AXIS) * 2 + which, ((z + dz) % AXIS) * AXIS + (y + dy) % AXIS

    peers = [(o, device(o, other), other) for o in OFFSETS for other in (1, 0) if other or hops(o)]
    for _, peer, _ in peers:
        pl.semaphore_signal(barrier, inc=1, device_id=peer, device_id_type=MESH)
    for load in loads:
        load.wait()

    keys, values = sorted_block(local[0], local[1])
    for ref in (sample, rows.at[me]):
        ref[...] = keys[SUBS - 1 :, :]
    for c, tile in enumerate((keys, values)):
        tile = packed(tile)
        block[c] = tile
        blocks[c, me] = tile
    pl.semaphore_wait(barrier, devices - 1)

    for _, peer, _ in peers:
        pltpu.make_async_remote_copy(
            src_ref=sample,
            dst_ref=rows.at[me],
            send_sem=row_send,
            recv_sem=row_recv,
            device_id=peer,
            device_id_type=MESH,
        ).start()
    for c in range(2):
        for (dx, dz, dy), peer, other in peers:
            if not other:
                pltpu.make_async_remote_copy(
                    src_ref=block.at[c],
                    dst_ref=blocks.at[c, me],
                    send_sem=send_sem.at[c],
                    recv_sem=recv_sem.at[c, (AXIS - dx) % AXIS],
                    device_id=peer,
                    device_id_type=MESH,
                ).start()

    def forward(c):
        gives = []
        for dx in (0, 1, 3, 2):
            at = (((x + dx) % AXIS) * 2 + core) * planes
            arrived = blocks.at[c, pl.ds(at, planes if dx else planes - 1)]
            pltpu.make_async_copy(arrived, arrived, recv_sem.at[c, dx]).wait()
            group = blocks.at[c, pl.ds(at, planes)]
            give = pltpu.make_async_remote_copy(
                src_ref=group,
                dst_ref=group,
                send_sem=give_sem.at[c, dx],
                recv_sem=take_sem.at[c, dx],
                device_id=(x * 2 + 1 - core, gy),
                device_id_type=MESH,
            )
            give.start()
            gives.append(give)
        return gives

    all_rows = rows.at[pl.ds(0, devices - 1)]
    pltpu.make_async_copy(all_rows, all_rows, row_recv).wait()
    wanted = [me * LANES, (me + 1) * LANES]
    zero = jnp.zeros((SUBS, LANES), i32)
    ends = search(rows, wanted, [zero] * 2, SHIFTS[:EARLY])
    key_gives = forward(0)
    low, high = search(rows, wanted, ends, SHIFTS[EARLY:])
    high = jnp.where(me == devices - 1, BIG, high)
    codes = group_plan(wanted, low, high, rows, turns, inside)
    tiles = collect([zero] * 2, blocks, 0, turns, inside, core)
    value_gives = forward(1)
    for give in key_gives:
        give.wait_recv()
    tiles = collect(tiles, blocks, 0, turns, inside, 1 - core)
    keys = bucket_keys(tiles, codes, low, high)
    ranks = candidate_ranks(keys)
    tiles = collect([zero] * 2, blocks, 1, turns, inside, core)
    for give in value_gives:
        give.wait_recv()
    tiles = collect(tiles, blocks, 1, turns, inside, 1 - core)
    for n, tile in enumerate(keys + [unpacked(t) for t in tiles] + ranks):
        found_ref[n * SUBS : (n + 1) * SUBS, :] = tile
    pltpu.make_async_copy(all_rows, all_rows, row_send).wait()
    for c in range(2):
        sent = blocks.at[c, pl.ds(0, AXIS * planes - 1)]
        pltpu.make_async_copy(sent, sent, send_sem.at[c]).wait()
    for give in key_gives + value_gives:
        give.wait_send()


SHIFTS = tuple(range(21, -1, -3))
EARLY = 4


def search(rows_ref, wanted, base, shifts):
    subs = iota((SUBS, LANES), 0)
    base = list(base)
    zero = jnp.zeros((SUBS, LANES), i32)
    for shift in shifts:
        tests = [b + ((subs + 1) << shift) for b in base]
        accs = [[zero, zero] for _ in tests]
        for r in range(LANES):
            one = jnp.broadcast_to(rows_ref[r], (SUBS, LANES))
            for n, test in enumerate(tests):
                accs[n][r % 2] = accs[n][r % 2] + jnp.where(one < test, 1, 0)
        for n in range(len(wanted)):
            below = jnp.sum((accs[n][0] + accs[n][1]).astype(f32), axis=1, keepdims=True)
            passed = jnp.where((below < wanted[n].astype(f32)) & (subs[:, :1] < SUBS - 1), 1, 0)
            digit = jnp.sum(passed, axis=0, keepdims=True)
            base[n] = base[n] + (jnp.broadcast_to(digit, (SUBS, LANES)) << shift)
    return base


def group_plan(wanted, low, high, rows_ref, turn_ref, in_ref):
    square = (LANES, LANES)
    samples = rows_ref[...].reshape(square)
    ends = [jnp.broadcast_to(k[:1, :], square) for k in (low, high)]
    ones = jnp.ones(square, bf16)
    below = jnp.where(iota(square, 1) < iota(square, 0), 1.0, 0.0).astype(bf16)

    def mm(a, b):
        return jnp.dot(a, b, preferred_element_type=f32)

    masks = []
    for k in ends:
        masks += [samples < k, samples <= k]
    counts = mm(jnp.concatenate([jnp.where(m, 1.0, 0.0).astype(bf16) for m in masks], axis=0), ones)
    counts = [counts[n * LANES : (n + 1) * LANES, :] for n in range(4)]
    taken, tied = [], []
    for n in range(2):
        lt, le = counts[2 * n], counts[2 * n + 1]
        equal = le - lt
        before = mm(below, equal.astype(bf16))
        total = mm(ones, lt.astype(bf16))
        left = jnp.asarray(wanted[n], f32) - total - before
        taken.append(lt + jnp.clip(left, 0.0, equal))
        tied.append(jnp.where(left > equal, 1, 0))
    first = taken[0]
    number = jnp.minimum(taken[1], LANES - 1.0) - first + 1.0
    start = mm(below, number.astype(bf16)).astype(i32)
    number, first, last = number.astype(i32), first.astype(i32), taken[1].astype(i32)
    lanes = iota(square, 1)
    turn_ref[...] = (lanes - (start - first)) & (LANES - 1)
    codes = []
    for h in range(2):
        m = lanes + h * LANES
        inside = (m >= start) & (m < start + number)
        in_ref[h] = jnp.where(inside, 1, 0)
        code = jnp.where(inside, 16, 0)
        code = code + jnp.where(inside & (m == start), 1 + tied[0], 0)
        code = code + jnp.where(inside & (m == start + last - first), 4 * (1 + tied[1]), 0)
        codes.append(code.astype(f32).astype(bf16))
    return mm(jnp.ones((SUBS, LANES), bf16), jnp.concatenate(codes, axis=1)).astype(i32)


def collect(tiles, blocks_ref, c, turn_ref, in_ref, core):
    tiles = list(tiles)
    planes = AXIS * AXIS
    empty = jnp.zeros((SUBS - SHORT, LANES), i32)
    for at in range(AXIS * planes):
        b = (at // planes * 2 + core) * planes + at % planes
        turn = jnp.broadcast_to(turn_ref[pl.ds(b, 1), :], (SUBS, LANES))
        tile = jnp.concatenate([blocks_ref[c, b], empty], axis=0)
        tile = jnp.take_along_axis(tile, turn, axis=1, mode="promise_in_bounds")
        for h in range(2):
            here = jnp.broadcast_to(in_ref[h, pl.ds(b, 1), :], (SUBS, LANES)) > 0
            tiles[h] = jnp.where(here, tile, tiles[h])
    return tiles


def bucket_keys(tiles, codes, low, high):
    keys = []
    for h, tile in enumerate(tiles):
        k = unpacked(tile)
        code = codes[:, h * LANES : (h + 1) * LANES]
        is_low, is_high = code & 3, (code >> 2) & 3
        ok = code >= 16
        ok = ok & ((is_low == 0) | (k >= low + is_low - 1))
        ok = ok & ((is_high == 0) | (k < high + is_high - 1))
        keys.append(jnp.where(ok, k, BIG))
    return keys


def place_kernel(found_ref, keys_out, values_out, size_out, digest_out):
    found = [found_ref[n * SUBS : (n + 1) * SUBS, :] for n in range(6)]
    keys, values, ranks = found[:2], found[2:4], found[4:]
    valid = jnp.where(keys[0] < BIG, 1, 0) + jnp.where(keys[1] < BIG, 1, 0)
    size = jnp.sum(jnp.sum(valid, axis=1, keepdims=True), axis=0, keepdims=True)
    count = 2 * SUBS
    keys, values = placed(
        list(zip(keys, values)), [r >> 7 for r in ranks], [r & (LANES - 1) for r in ranks], count
    )
    rank = iota((count, LANES), 0) * LANES + iota((count, LANES), 1)
    filled = rank < size
    keys = jnp.where(filled, keys, -1)
    values = jnp.where(filled, values, -1)
    keys_out[...] = keys[: keys_out.shape[0], :]
    values_out[...] = values[: values_out.shape[0], :]
    mixed = (keys + 3 * values + 5 * rank) & 1023
    digest = jnp.where(filled, 2 * mixed - 1023, 0)
    digest = jnp.sum(jnp.sum(digest, axis=1, keepdims=True), axis=0, keepdims=True)
    size_out[0] = size[0, 0]
    digest_out[0] = digest[0, 0]


def candidates(keys, values):
    dma = pltpu.SemaphoreType.DMA
    return pl.pallas_call(
        gather_kernel,
        out_shape=jax.ShapeDtypeStruct((6 * SUBS, LANES), i32),
        in_specs=[pl.BlockSpec(memory_space=pltpu.HBM)] * 2,
        out_specs=pl.BlockSpec(memory_space=pltpu.VMEM),
        scratch_shapes=[
            pltpu.VMEM((2, SUBS, LANES), i32),
            pltpu.VMEM((1, LANES), i32),
            pltpu.VMEM((2, SHORT, LANES), i32),
            pltpu.VMEM((LANES, 1, LANES), i32),
            pltpu.VMEM((2, LANES, SHORT, LANES), i32),
            pltpu.VMEM((LANES, LANES), i32),
            pltpu.VMEM((2, LANES, LANES), i32),
            dma((2,)),
            dma,
            dma,
            dma((2,)),
            dma((2, AXIS)),
            dma((2, AXIS)),
            dma((2, AXIS)),
        ],
        compiler_params=pltpu.CompilerParams(collective_id=0, has_side_effects=True, vmem_limit_bytes=8 << 20),
        name="find_candidates",
    )(keys, values)


def placed_bucket(found, rows):
    one = jax.ShapeDtypeStruct((1,), i32)
    return pl.pallas_call(
        place_kernel,
        out_shape=(jax.ShapeDtypeStruct((rows, LANES), i32),) * 2 + (one, one),
        in_specs=[pl.BlockSpec(memory_space=pltpu.VMEM)],
        out_specs=[pl.BlockSpec(memory_space=pltpu.VMEM)] * 2 + [pl.BlockSpec(memory_space=pltpu.SMEM)] * 2,
        compiler_params=pltpu.CompilerParams(vmem_limit_bytes=8 << 20),
        name="place_bucket",
    )(found)


def solution(mesh):
    gx, gy = mesh.shape["gx"], mesh.shape["gy"]

    def shards(record_keys, payloads):
        keys = record_keys.reshape(SUBS, LANES)
        values = payloads.reshape(SUBS, LANES)
        keys, values = (pltpu.with_memory_space_constraint(a, pltpu.HBM) for a in (keys, values))
        found = candidates(keys, values)
        rows = (2 * record_keys.shape[0] - gx * gy) // LANES
        sorted_keys, sorted_values, size, digest = placed_bucket(found, rows)
        return sorted_keys.reshape(-1), sorted_values.reshape(-1), size, digest

    spec = P(("gx", "gy"))
    return jax.shard_map(shards, mesh=mesh, in_specs=(spec,) * 2, out_specs=(spec,) * 4, check_vma=False)
```

```python
import functools

import jax
import jax.numpy as jnp
from jax import lax
from jax.experimental import pallas as pl
from jax.experimental.pallas import tpu as pltpu
from jax.sharding import PartitionSpec as P

MESH = pl.DeviceIdType.MESH
LANES = 128
SUBS = 8
CHUNK = 256
CHUNKS = 3
BIG = 1 << 24
f32, bf16, i32 = jnp.float32, jnp.bfloat16, jnp.int32


def iota(shape, dim):
    return lax.broadcasted_iota(i32, shape, dim)


def row(x, s):
    return jnp.broadcast_to(x[s : s + 1, :], (SUBS, LANES))


def pieces(x):
    return [x & (CHUNK - 1), (x >> 8) & (CHUNK - 1), x >> 16]


def joined(parts):
    parts = [p.astype(i32) for p in parts]
    return parts[0] + (parts[1] << 8) + (parts[2] << 16)


def placed(rows, his, los, count):
    left, right = [], []
    for (keys, values), hi, lo in zip(rows, his, los):
        parts = [p.astype(f32) for p in pieces(keys) + pieces(values)]
        for s in range(SUBS):
            onehot = jnp.broadcast_to(lo[s : s + 1, :], (LANES, LANES)) == iota((LANES, LANES), 0)
            right.append(jnp.where(onehot, 1.0, 0.0).astype(bf16))
            column = []
            at = jnp.broadcast_to(hi[s : s + 1, :], (count, LANES)) == iota((count, LANES), 0)
            for p in parts:
                column.append(jnp.where(at, jnp.broadcast_to(p[s : s + 1, :], (count, LANES)), 0.0))
            left.append(jnp.concatenate(column, axis=0).astype(bf16))
    left = jnp.concatenate(left, axis=1)
    right = jnp.concatenate(right, axis=1)
    out = lax.dot_general(left, right, (((1,), (1,)), ((), ())), preferred_element_type=f32)
    out = [out[c * count : (c + 1) * count, :] for c in range(2 * CHUNKS)]
    return joined(out[:CHUNKS]), joined(out[CHUNKS:])


def sublane_sums(accs):
    return jnp.concatenate([jnp.sum(a, axis=0, keepdims=True) for a in accs], axis=0)


def column(x, m):
    return jnp.broadcast_to(x[:, m : m + 1], (SUBS, LANES))


def block_ranks(keys):
    subs, lanes = iota((SUBS, LANES), 0), iota((SUBS, LANES), 1)
    rows = [row(keys, s) + jnp.where(subs < s, 1, 0) for s in range(SUBS)]
    zero = jnp.zeros((SUBS, LANES), i32)
    accs, ties = [zero] * SUBS, zero
    for m in range(LANES):
        one = column(keys, m)
        for s in range(SUBS):
            accs[s] = accs[s] + jnp.where(one < rows[s], 1, 0)
        ties = ties + jnp.where((one == keys) & (lanes > m), 1, 0)
    return sublane_sums(accs) + ties


def candidate_ranks(halves):
    subs, lanes = iota((SUBS, LANES), 0), iota((SUBS, LANES), 1)
    zero = jnp.zeros((SUBS, LANES), i32)
    width = LANES // SUBS
    spread = (lanes + width * subs) & (LANES - 1)
    tables = [
        [jnp.take_along_axis(row(k, s), spread, axis=1, mode="promise_in_bounds") for s in range(SUBS)] for k in halves
    ]
    dropped = sum(jnp.where(k < 0, 1, 0) for k in halves)
    dropped = jnp.sum(jnp.sum(dropped, axis=1, keepdims=True), axis=0, keepdims=True)
    ranks = []
    for target, keys in enumerate(halves):
        rows = [row(keys, s) for s in range(SUBS)]
        accs = [zero] * SUBS
        for source, table in enumerate(tables):
            if target > source:
                table = [t - 1 for t in table]
            for m in range(width):
                ones = [column(t, m) for t in table]
                if target == source:
                    after = jnp.where(lanes > m + width * subs, 1, 0)
                    ones = [one - after for one in ones]
                for r in range(SUBS):
                    count = jnp.where(ones[0] < rows[r], 1, 0)
                    for s in range(1, SUBS):
                        count = jnp.where(ones[s] < rows[r], s + 1, count)
                    accs[r] = accs[r] + count
        ties = zero
        for d in range(1, SUBS):
            ties = ties + jnp.where((pltpu.roll(keys, d, 0) == keys) & (subs >= d), 1, 0)
        rank = sublane_sums(accs) + ties - dropped
        ranks.append(jnp.where((keys >= 0) & (keys < BIG), rank, 2 * SUBS * LANES - 1))
    return ranks


def sorted_block(keys, values):
    rank = block_ranks(keys)
    return placed([(keys, values)], [rank & (SUBS - 1)], [rank >> 3], SUBS)


SHORT = 6
BYTE = 24
AXIS = 4


def packed(x):
    extra = [(x[SHORT + r // 3 : SHORT + r // 3 + 1, :] >> (8 * (r % 3))) & 255 for r in range(SHORT)]
    return x[:SHORT, :] | (jnp.concatenate(extra, axis=0) << BYTE)


def unpacked(x):
    extra = (x >> BYTE) & 255
    last = [extra[r : r + 1, :] | (extra[r + 1 : r + 2, :] << 8) | (extra[r + 2 : r + 3, :] << 16) for r in (0, 3)]
    return jnp.concatenate([x[:SHORT, :] & (BIG - 1)] + last, axis=0)


def hops(offset):
    return sum(min(k, AXIS - k) for k in offset)


OFFSETS = sorted(((dx, dz, dy) for dx in range(AXIS) for dz in range(AXIS) for dy in range(AXIS)), key=lambda o: -hops(o))


def gather_kernel(
    keys_hbm,
    values_hbm,
    found_ref,
    local,
    sample,
    block,
    rows,
    blocks,
    turns,
    inside,
    local_sem,
    row_send,
    row_recv,
    row_give,
    row_take,
    send_sem,
    recv_sem,
    give_sem,
    take_sem,
):
    gx, gy = lax.axis_index("gx"), lax.axis_index("gy")
    x, core, z, y = gx // 2, gx % 2, gy // AXIS, gy % AXIS
    planes = AXIS * AXIS
    devices = 2 * AXIS * planes
    me = gx * planes + gy
    barrier = pltpu.get_barrier_semaphore()
    loads = [pltpu.make_async_copy(ref, local.at[c], local_sem.at[c]) for c, ref in enumerate((keys_hbm, values_hbm))]
    for load in loads:
        load.start()

    def device(offset):
        dx, dz, dy = offset
        return ((x + dx) % AXIS) * 2 + core, ((z + dz) % AXIS) * AXIS + (y + dy) % AXIS

    peers = [(o, device(o)) for o in OFFSETS if hops(o)]
    partner = (x * 2 + 1 - core, gy)
    for _, peer in peers + [(None, partner)]:
        pl.semaphore_signal(barrier, inc=1, device_id=peer, device_id_type=MESH)
    for load in loads:
        load.wait()

    keys, values = sorted_block(local[0], local[1])
    for ref in (sample, rows.at[me]):
        ref[...] = keys[SUBS - 1 :, :]
    for c, tile in enumerate((keys, values)):
        tile = packed(tile)
        block[c] = tile
        blocks[c, me] = tile
    pl.semaphore_wait(barrier, AXIS * planes)

    for _, peer in peers:
        pltpu.make_async_remote_copy(
            src_ref=sample,
            dst_ref=rows.at[me],
            send_sem=row_send,
            recv_sem=row_recv,
            device_id=peer,
            device_id_type=MESH,
        ).start()
    for c in range(2):
        for (dx, dz, dy), peer in peers:
            pltpu.make_async_remote_copy(
                src_ref=block.at[c],
                dst_ref=blocks.at[c, me],
                send_sem=send_sem.at[c],
                recv_sem=recv_sem.at[c, (AXIS - dx) % AXIS],
                device_id=peer,
                device_id_type=MESH,
            ).start()

    def forward(c):
        gives = []
        for dx in (0, 1, 3, 2):
            at = (((x + dx) % AXIS) * 2 + core) * planes
            arrived = blocks.at[c, pl.ds(at, planes if dx else planes - 1)]
            pltpu.make_async_copy(arrived, arrived, recv_sem.at[c, dx]).wait()
            group = blocks.at[c, pl.ds(at, planes)]
            give = pltpu.make_async_remote_copy(
                src_ref=group,
                dst_ref=group,
                send_sem=give_sem.at[c, dx],
                recv_sem=take_sem.at[c, dx],
                device_id=partner,
                device_id_type=MESH,
            )
            give.start()
            gives.append(give)
        return gives

    some_rows = rows.at[pl.ds(0, AXIS * planes - 1)]
    pltpu.make_async_copy(some_rows, some_rows, row_recv).wait()
    for dx in range(AXIS):
        group = rows.at[pl.ds(((x + dx) % AXIS * 2 + core) * planes, planes)]
        pltpu.make_async_remote_copy(
            src_ref=group,
            dst_ref=group,
            send_sem=row_give,
            recv_sem=row_take,
            device_id=partner,
            device_id_type=MESH,
        ).start()
    half_rows = rows.at[pl.ds(0, AXIS * planes)]
    pltpu.make_async_copy(half_rows, half_rows, row_take).wait()
    wanted = [me * LANES, (me + 1) * LANES]
    zero = jnp.zeros((SUBS, LANES), i32)
    ends = search(rows, wanted, [zero] * 2, SHIFTS[:EARLY])
    key_gives = forward(0)
    low, high = search(rows, wanted, ends, SHIFTS[EARLY:])
    high = jnp.where(me == devices - 1, BIG, high)
    codes = group_plan(wanted, low, high, rows, turns, inside)
    tiles = collect([zero] * 2, blocks, 0, turns, inside, core)
    value_gives = forward(1)
    for give in key_gives:
        give.wait_recv()
    tiles = collect(tiles, blocks, 0, turns, inside, 1 - core)
    keys = bucket_keys(tiles, codes, low, high)
    ranks = candidate_ranks(keys)
    tiles = collect([zero] * 2, blocks, 1, turns, inside, core)
    for give in value_gives:
        give.wait_recv()
    tiles = collect(tiles, blocks, 1, turns, inside, 1 - core)
    for n, tile in enumerate(keys + [unpacked(t) for t in tiles] + ranks):
        found_ref[n * SUBS : (n + 1) * SUBS, :] = tile
    pltpu.make_async_copy(some_rows, some_rows, row_send).wait()
    pltpu.make_async_copy(half_rows, half_rows, row_give).wait()
    for c in range(2):
        sent = blocks.at[c, pl.ds(0, AXIS * planes - 1)]
        pltpu.make_async_copy(sent, sent, send_sem.at[c]).wait()
    for give in key_gives + value_gives:
        give.wait_send()


SHIFTS = tuple(range(21, -1, -3))
EARLY = 4


def search(rows_ref, wanted, base, shifts):
    subs = iota((SUBS, LANES), 0)
    base = list(base)
    zero = jnp.zeros((SUBS, LANES), i32)
    for shift in shifts:
        tests = [b + ((subs + 1) << shift) for b in base]
        accs = [[zero, zero] for _ in tests]
        for r in range(LANES):
            one = jnp.broadcast_to(rows_ref[r], (SUBS, LANES))
            for n, test in enumerate(tests):
                accs[n][r % 2] = accs[n][r % 2] + jnp.where(one < test, 1, 0)
        for n in range(len(wanted)):
            below = jnp.broadcast_to(jnp.sum((accs[n][0] + accs[n][1]).astype(f32), axis=1, keepdims=True), (SUBS, LANES))
            passed = jnp.where((below < wanted[n].astype(f32)) & (subs < SUBS - 1), 1, 0)
            for turn in (4, 2, 1):
                passed = passed + pltpu.roll(passed, turn, 0)
            base[n] = base[n] + (passed << shift)
    return base


def group_plan(wanted, low, high, rows_ref, turn_ref, in_ref):
    square = (LANES, LANES)
    samples = rows_ref[...].reshape(square)
    ends = [jnp.broadcast_to(k[:1, :], square) for k in (low, high)]
    ones = jnp.ones(square, bf16)
    below = jnp.where(iota(square, 1) < iota(square, 0), 1.0, 0.0).astype(bf16)

    def mm(a, b):
        return jnp.dot(a, b, preferred_element_type=f32)

    masks = []
    for k in ends:
        masks += [samples < k, samples <= k]
    counts = mm(jnp.concatenate([jnp.where(m, 1.0, 0.0).astype(bf16) for m in masks], axis=0), ones)
    counts = [counts[n * LANES : (n + 1) * LANES, :] for n in range(4)]
    taken, tied = [], []
    for n in range(2):
        lt, le = counts[2 * n], counts[2 * n + 1]
        equal = le - lt
        before = mm(below, equal.astype(bf16))
        total = mm(ones, lt.astype(bf16))
        left = jnp.asarray(wanted[n], f32) - total - before
        taken.append(lt + jnp.clip(left, 0.0, equal))
        tied.append(jnp.where(left > equal, 1, 0))
    first = taken[0]
    number = jnp.minimum(taken[1], LANES - 1.0) - first + 1.0
    start = mm(below, number.astype(bf16)).astype(i32)
    number, first, last = number.astype(i32), first.astype(i32), taken[1].astype(i32)
    lanes = iota(square, 1)
    turn_ref[...] = (lanes - (start - first)) & (LANES - 1)
    codes = []
    for h in range(2):
        m = lanes + h * LANES
        inside = (m >= start) & (m < start + number)
        in_ref[h] = jnp.where(inside, 1, 0)
        code = jnp.where(inside, 16, 0)
        code = code + jnp.where(inside & (m == start), 1 + tied[0], 0)
        code = code + jnp.where(inside & (m == start + last - first), 4 * (1 + tied[1]), 0)
        codes.append(code.astype(f32).astype(bf16))
    return mm(jnp.ones((SUBS, LANES), bf16), jnp.concatenate(codes, axis=1)).astype(i32)


def collect(tiles, blocks_ref, c, turn_ref, in_ref, core):
    tiles = list(tiles)
    planes = AXIS * AXIS
    empty = jnp.zeros((SUBS - SHORT, LANES), i32)
    for at in range(AXIS * planes):
        b = (at // planes * 2 + core) * planes + at % planes
        turn = jnp.broadcast_to(turn_ref[pl.ds(b, 1), :], (SUBS, LANES))
        tile = jnp.concatenate([blocks_ref[c, b], empty], axis=0)
        tile = jnp.take_along_axis(tile, turn, axis=1, mode="promise_in_bounds")
        for h in range(2):
            here = jnp.broadcast_to(in_ref[h, pl.ds(b, 1), :], (SUBS, LANES)) > 0
            tiles[h] = jnp.where(here, tile, tiles[h])
    return tiles


def bucket_keys(tiles, codes, low, high):
    keys = []
    for h, tile in enumerate(tiles):
        k = unpacked(tile)
        code = codes[:, h * LANES : (h + 1) * LANES]
        is_low, is_high = code & 3, (code >> 2) & 3
        over = (code < 16) | ((is_high > 0) & (k >= high + is_high - 1))
        under = (is_low > 0) & (k < low + is_low - 1)
        keys.append(jnp.where(over, BIG, jnp.where(under, -1, k)))
    return keys


def place_kernel(found_ref, keys_out, values_out, size_out, digest_out):
    found = [found_ref[n * SUBS : (n + 1) * SUBS, :] for n in range(6)]
    keys, values, ranks = found[:2], found[2:4], found[4:]
    valid = sum(jnp.where((k >= 0) & (k < BIG), 1, 0) for k in keys)
    size = jnp.sum(jnp.sum(valid, axis=1, keepdims=True), axis=0, keepdims=True)
    count = 2 * SUBS
    keys, values = placed(
        list(zip(keys, values)), [r >> 7 for r in ranks], [r & (LANES - 1) for r in ranks], count
    )
    rank = iota((count, LANES), 0) * LANES + iota((count, LANES), 1)
    filled = rank < size
    keys = jnp.where(filled, keys, -1)
    values = jnp.where(filled, values, -1)
    keys_out[...] = keys[: keys_out.shape[0], :]
    values_out[...] = values[: values_out.shape[0], :]
    mixed = (keys + 3 * values + 5 * rank) & 1023
    digest = jnp.where(filled, 2 * mixed - 1023, 0)
    digest = jnp.sum(jnp.sum(digest, axis=1, keepdims=True), axis=0, keepdims=True)
    size_out[0] = size[0, 0]
    digest_out[0] = digest[0, 0]


def candidates(keys, values):
    dma = pltpu.SemaphoreType.DMA
    return pl.pallas_call(
        gather_kernel,
        out_shape=jax.ShapeDtypeStruct((6 * SUBS, LANES), i32),
        in_specs=[pl.BlockSpec(memory_space=pltpu.HBM)] * 2,
        out_specs=pl.BlockSpec(memory_space=pltpu.VMEM),
        scratch_shapes=[
            pltpu.VMEM((2, SUBS, LANES), i32),
            pltpu.VMEM((1, LANES), i32),
            pltpu.VMEM((2, SHORT, LANES), i32),
            pltpu.VMEM((LANES, 1, LANES), i32),
            pltpu.VMEM((2, LANES, SHORT, LANES), i32),
            pltpu.VMEM((LANES, LANES), i32),
            pltpu.VMEM((2, LANES, LANES), i32),
            dma((2,)),
            dma,
            dma,
            dma,
            dma,
            dma((2,)),
            dma((2, AXIS)),
            dma((2, AXIS)),
            dma((2, AXIS)),
        ],
        compiler_params=pltpu.CompilerParams(collective_id=0, has_side_effects=True, vmem_limit_bytes=8 << 20),
        name="find_candidates",
    )(keys, values)


def placed_bucket(found, rows):
    one = jax.ShapeDtypeStruct((1,), i32)
    return pl.pallas_call(
        place_kernel,
        out_shape=(jax.ShapeDtypeStruct((rows, LANES), i32),) * 2 + (one, one),
        in_specs=[pl.BlockSpec(memory_space=pltpu.VMEM)],
        out_specs=[pl.BlockSpec(memory_space=pltpu.VMEM)] * 2 + [pl.BlockSpec(memory_space=pltpu.SMEM)] * 2,
        compiler_params=pltpu.CompilerParams(vmem_limit_bytes=8 << 20),
        name="place_bucket",
    )(found)


def solution(mesh):
    gx, gy = mesh.shape["gx"], mesh.shape["gy"]

    def shards(record_keys, payloads):
        keys = record_keys.reshape(SUBS, LANES)
        values = payloads.reshape(SUBS, LANES)
        keys, values = (pltpu.with_memory_space_constraint(a, pltpu.HBM) for a in (keys, values))
        found = candidates(keys, values)
        rows = (2 * record_keys.shape[0] - gx * gy) // LANES
        sorted_keys, sorted_values, size, digest = placed_bucket(found, rows)
        return sorted_keys.reshape(-1), sorted_values.reshape(-1), size, digest

    spec = P(("gx", "gy"))
    return jax.shard_map(shards, mesh=mesh, in_specs=(spec,) * 2, out_specs=(spec,) * 4, check_vma=False)
```

```python
import functools

import jax
import jax.numpy as jnp
from jax import lax
from jax.experimental import pallas as pl
from jax.experimental.pallas import tpu as pltpu
from jax.sharding import PartitionSpec as P

MESH = pl.DeviceIdType.MESH
LANES = 128
SUBS = 8
CHUNK = 256
CHUNKS = 3
BIG = 1 << 24
f32, bf16, i32 = jnp.float32, jnp.bfloat16, jnp.int32


def iota(shape, dim):
    return lax.broadcasted_iota(i32, shape, dim)


def row(x, s):
    return jnp.broadcast_to(x[s : s + 1, :], (SUBS, LANES))


def pieces(x):
    return [x & (CHUNK - 1), (x >> 8) & (CHUNK - 1), x >> 16]


def joined(parts):
    parts = [p.astype(i32) for p in parts]
    return parts[0] + (parts[1] << 8) + (parts[2] << 16)


def placed(rows, his, los, count):
    left, right = [], []
    for (keys, values), hi, lo in zip(rows, his, los):
        parts = [p.astype(f32) for p in pieces(keys) + pieces(values)]
        for s in range(SUBS):
            onehot = jnp.broadcast_to(lo[s : s + 1, :], (LANES, LANES)) == iota((LANES, LANES), 0)
            right.append(jnp.where(onehot, 1.0, 0.0).astype(bf16))
            column = []
            at = jnp.broadcast_to(hi[s : s + 1, :], (count, LANES)) == iota((count, LANES), 0)
            for p in parts:
                column.append(jnp.where(at, jnp.broadcast_to(p[s : s + 1, :], (count, LANES)), 0.0))
            left.append(jnp.concatenate(column, axis=0).astype(bf16))
    left = jnp.concatenate(left, axis=1)
    right = jnp.concatenate(right, axis=1)
    out = lax.dot_general(left, right, (((1,), (1,)), ((), ())), preferred_element_type=f32)
    out = [out[c * count : (c + 1) * count, :] for c in range(2 * CHUNKS)]
    return joined(out[:CHUNKS]), joined(out[CHUNKS:])


def sublane_sums(accs):
    return jnp.concatenate([jnp.sum(a, axis=0, keepdims=True) for a in accs], axis=0)


def column(x, m):
    return jnp.broadcast_to(x[:, m : m + 1], (SUBS, LANES))


def block_ranks(keys):
    subs, lanes = iota((SUBS, LANES), 0), iota((SUBS, LANES), 1)
    rows = [row(keys, s) + jnp.where(subs < s, 1, 0) for s in range(SUBS)]
    zero = jnp.zeros((SUBS, LANES), i32)
    accs, ties = [zero] * SUBS, zero
    for m in range(LANES):
        one = column(keys, m)
        for s in range(SUBS):
            accs[s] = accs[s] + jnp.where(one < rows[s], 1, 0)
        ties = ties + jnp.where((one == keys) & (lanes > m), 1, 0)
    return sublane_sums(accs) + ties


def candidate_ranks(halves):
    subs, lanes = iota((SUBS, LANES), 0), iota((SUBS, LANES), 1)
    zero = jnp.zeros((SUBS, LANES), i32)
    width = LANES // SUBS
    spread = (lanes + width * subs) & (LANES - 1)
    tables = [
        [jnp.take_along_axis(row(k, s), spread, axis=1, mode="promise_in_bounds") for s in range(SUBS)] for k in halves
    ]
    dropped = sum(jnp.where(k < 0, 1, 0) for k in halves)
    dropped = jnp.sum(jnp.sum(dropped, axis=1, keepdims=True), axis=0, keepdims=True)
    ranks = []
    for target, keys in enumerate(halves):
        rows = [row(keys, s) for s in range(SUBS)]
        accs = [zero] * SUBS
        for source, table in enumerate(tables):
            if target > source:
                table = [t - 1 for t in table]
            for m in range(width):
                ones = [column(t, m) for t in table]
                if target == source:
                    after = jnp.where(lanes > m + width * subs, 1, 0)
                    ones = [one - after for one in ones]
                for r in range(SUBS):
                    count = jnp.where(ones[0] < rows[r], 1, 0)
                    for s in range(1, SUBS):
                        count = jnp.where(ones[s] < rows[r], s + 1, count)
                    accs[r] = accs[r] + count
        ties = zero
        for d in range(1, SUBS):
            ties = ties + jnp.where((pltpu.roll(keys, d, 0) == keys) & (subs >= d), 1, 0)
        rank = sublane_sums(accs) + ties - dropped
        ranks.append(jnp.where((keys >= 0) & (keys < BIG), rank, 2 * SUBS * LANES - 1))
    return ranks


def sorted_block(keys, values):
    rank = block_ranks(keys)
    return placed([(keys, values)], [rank & (SUBS - 1)], [rank >> 3], SUBS)


SHORT = 6
BYTE = 24
AXIS = 4


def packed(x):
    extra = [(x[SHORT + r // 3 : SHORT + r // 3 + 1, :] >> (8 * (r % 3))) & 255 for r in range(SHORT)]
    return x[:SHORT, :] | (jnp.concatenate(extra, axis=0) << BYTE)


def unpacked(x):
    extra = (x >> BYTE) & 255
    last = [extra[r : r + 1, :] | (extra[r + 1 : r + 2, :] << 8) | (extra[r + 2 : r + 3, :] << 16) for r in (0, 3)]
    return jnp.concatenate([x[:SHORT, :] & (BIG - 1)] + last, axis=0)


def hops(offset):
    return sum(min(k, AXIS - k) for k in offset)


OFFSETS = sorted(((dx, dz, dy) for dx in range(AXIS) for dz in range(AXIS) for dy in range(AXIS)), key=lambda o: -hops(o))


def gather_kernel(
    keys_hbm,
    values_hbm,
    found_ref,
    local,
    sample,
    block,
    rows,
    blocks,
    turns,
    inside,
    local_sem,
    row_send,
    row_recv,
    row_give,
    row_take,
    send_sem,
    recv_sem,
    give_sem,
    take_sem,
):
    gx, gy = lax.axis_index("gx"), lax.axis_index("gy")
    x, core, z, y = gx // 2, gx % 2, gy // AXIS, gy % AXIS
    planes = AXIS * AXIS
    devices = 2 * AXIS * planes
    me = gx * planes + gy
    barrier = pltpu.get_barrier_semaphore()
    loads = [pltpu.make_async_copy(ref, local.at[c], local_sem.at[c]) for c, ref in enumerate((keys_hbm, values_hbm))]
    for load in loads:
        load.start()

    def device(offset):
        dx, dz, dy = offset
        return ((x + dx) % AXIS) * 2 + core, ((z + dz) % AXIS) * AXIS + (y + dy) % AXIS

    peers = [(o, device(o)) for o in OFFSETS if hops(o)]
    partner = (x * 2 + 1 - core, gy)
    for _, peer in peers + [(None, partner)]:
        pl.semaphore_signal(barrier, inc=1, device_id=peer, device_id_type=MESH)
    for load in loads:
        load.wait()

    keys, values = sorted_block(local[0], local[1])
    for ref in (sample, rows.at[me]):
        ref[...] = keys[SUBS - 1 :, :]
    for c, tile in enumerate((keys, values)):
        tile = packed(tile)
        block[c] = tile
        blocks[c, me] = tile
    pl.semaphore_wait(barrier, AXIS * planes)

    for _, peer in peers:
        pltpu.make_async_remote_copy(
            src_ref=sample,
            dst_ref=rows.at[me],
            send_sem=row_send,
            recv_sem=row_recv,
            device_id=peer,
            device_id_type=MESH,
        ).start()
    for c in range(2):
        for (dx, dz, dy), peer in peers:
            pltpu.make_async_remote_copy(
                src_ref=block.at[c],
                dst_ref=blocks.at[c, me],
                send_sem=send_sem.at[c],
                recv_sem=recv_sem.at[c, (AXIS - dx) % AXIS],
                device_id=peer,
                device_id_type=MESH,
            ).start()

    def forward(c):
        gives = []
        for dx in (0, 1, 3, 2):
            at = (((x + dx) % AXIS) * 2 + core) * planes
            arrived = blocks.at[c, pl.ds(at, planes if dx else planes - 1)]
            pltpu.make_async_copy(arrived, arrived, recv_sem.at[c, dx]).wait()
            group = blocks.at[c, pl.ds(at, planes)]
            give = pltpu.make_async_remote_copy(
                src_ref=group,
                dst_ref=group,
                send_sem=give_sem.at[c, dx],
                recv_sem=take_sem.at[c, dx],
                device_id=partner,
                device_id_type=MESH,
            )
            give.start()
            gives.append(give)
        return gives

    some_rows = rows.at[pl.ds(0, AXIS * planes - 1)]
    pltpu.make_async_copy(some_rows, some_rows, row_recv).wait()
    for dx in range(AXIS):
        group = rows.at[pl.ds(((x + dx) % AXIS * 2 + core) * planes, planes)]
        pltpu.make_async_remote_copy(
            src_ref=group,
            dst_ref=group,
            send_sem=row_give,
            recv_sem=row_take,
            device_id=partner,
            device_id_type=MESH,
        ).start()
    half_rows = rows.at[pl.ds(0, AXIS * planes)]
    pltpu.make_async_copy(half_rows, half_rows, row_take).wait()
    wanted = [me * LANES, (me + 1) * LANES]
    zero = jnp.zeros((SUBS, LANES), i32)
    ends = search(rows, wanted, [zero] * 2, SHIFTS[:EARLY])
    key_gives = forward(0)
    low, high = search(rows, wanted, ends, SHIFTS[EARLY:])
    high = jnp.where(me == devices - 1, BIG, high)
    plan = group_plan(wanted, low, high, rows, turns, inside)
    tiles = collect([zero] * 2, blocks, 0, turns, inside, core)
    codes = column_codes(plan, inside)
    value_gives = forward(1)
    for give in key_gives:
        give.wait_recv()
    tiles = collect(tiles, blocks, 0, turns, inside, 1 - core)
    keys = bucket_keys(tiles, codes, low, high)
    ranks = candidate_ranks(keys)
    tiles = collect([zero] * 2, blocks, 1, turns, inside, core)
    for give in value_gives:
        give.wait_recv()
    tiles = collect(tiles, blocks, 1, turns, inside, 1 - core)
    for n, tile in enumerate(keys + [unpacked(t) for t in tiles] + ranks):
        found_ref[n * SUBS : (n + 1) * SUBS, :] = tile
    pltpu.make_async_copy(some_rows, some_rows, row_send).wait()
    pltpu.make_async_copy(half_rows, half_rows, row_give).wait()
    for c in range(2):
        sent = blocks.at[c, pl.ds(0, AXIS * planes - 1)]
        pltpu.make_async_copy(sent, sent, send_sem.at[c]).wait()
    for give in key_gives + value_gives:
        give.wait_send()


SHIFTS = tuple(range(21, -1, -3))
EARLY = 4


def search(rows_ref, wanted, base, shifts):
    subs = iota((SUBS, LANES), 0)
    base = list(base)
    zero = jnp.zeros((SUBS, LANES), i32)
    for shift in shifts:
        tests = [b + ((subs + 1) << shift) for b in base]
        accs = [[zero, zero] for _ in tests]
        for r in range(LANES):
            one = jnp.broadcast_to(rows_ref[r], (SUBS, LANES))
            for n, test in enumerate(tests):
                accs[n][r % 2] = accs[n][r % 2] + jnp.where(one < test, 1, 0)
        for n in range(len(wanted)):
            below = jnp.broadcast_to(jnp.sum((accs[n][0] + accs[n][1]).astype(f32), axis=1, keepdims=True), (SUBS, LANES))
            passed = jnp.where((below < wanted[n].astype(f32)) & (subs < SUBS - 1), 1, 0)
            for turn in (4, 2, 1):
                passed = passed + pltpu.roll(passed, turn, 0)
            base[n] = base[n] + (passed << shift)
    return base


def mm(a, b):
    return jnp.dot(a, b, preferred_element_type=f32)


def group_plan(wanted, low, high, rows_ref, turn_ref, in_ref):
    square = (LANES, LANES)
    samples = rows_ref[...].reshape(square)
    ones = jnp.ones(square, bf16)
    below = jnp.where(iota(square, 1) < iota(square, 0), 1.0, 0.0).astype(bf16)
    masks = []
    for k in (low, high):
        k = jnp.broadcast_to(k[:1, :], square)
        masks += [samples < k, samples == k]
    counts = mm(jnp.concatenate([jnp.where(m, 1.0, 0.0).astype(bf16) for m in masks], axis=0), ones)
    counts = [counts[n * LANES : (n + 1) * LANES, :] for n in range(4)]
    left_hand = jnp.concatenate([below, ones[: 2 * SUBS, :]], axis=0)
    sums = mm(left_hand, jnp.concatenate(counts, axis=1).astype(bf16))
    taken, tied, before = [], [], []
    for n in range(2):
        less, equal = counts[2 * n], counts[2 * n + 1]
        less_before, equal_before = (sums[:LANES, c * LANES : (c + 1) * LANES] for c in (2 * n, 2 * n + 1))
        total = jnp.broadcast_to(sums[LANES : LANES + 1, 2 * n * LANES : (2 * n + 1) * LANES], square)
        ties = jnp.asarray(wanted[n], f32) - total
        left = ties - equal_before
        taken.append((less + jnp.clip(left, 0.0, equal)).astype(i32))
        tied.append(jnp.where(left > equal, 1, 0))
        before.append(less_before + jnp.minimum(ties, equal_before))
    first, last = taken
    start = (before[1] - before[0]).astype(i32) + iota(square, 0)
    lanes = iota(square, 1)
    turn_ref[...] = (lanes - (start - first)) & (LANES - 1)
    for h in range(2):
        m = lanes + h * LANES
        in_ref[h] = jnp.where((m >= start) & (m <= start + last - first), 1, 0)
    return start, first, last, tied


def column_codes(plan, in_ref):
    start, first, last, tied = plan
    lanes = iota((LANES, LANES), 1)
    codes = []
    for h in range(2):
        m = lanes + h * LANES
        inside = (in_ref[h] > 0) & (m - start + first < LANES)
        code = jnp.where(m == start, 17 + tied[0], 16) + jnp.where(m == start + last - first, 4 * (1 + tied[1]), 0)
        codes.append(jnp.where(inside, code, 0).astype(f32).astype(bf16))
    return mm(jnp.ones((SUBS, LANES), bf16), jnp.concatenate(codes, axis=1)).astype(i32)


def collect(tiles, blocks_ref, c, turn_ref, in_ref, core):
    tiles = list(tiles)
    planes = AXIS * AXIS
    empty = jnp.zeros((SUBS - SHORT, LANES), i32)
    for at in range(AXIS * planes):
        b = (at // planes * 2 + core) * planes + at % planes
        turn = jnp.broadcast_to(turn_ref[pl.ds(b, 1), :], (SUBS, LANES))
        tile = jnp.concatenate([blocks_ref[c, b], empty], axis=0)
        tile = jnp.take_along_axis(tile, turn, axis=1, mode="promise_in_bounds")
        for h in range(2):
            here = jnp.broadcast_to(in_ref[h, pl.ds(b, 1), :], (SUBS, LANES)) > 0
            tiles[h] = jnp.where(here, tile, tiles[h])
    return tiles


def bucket_keys(tiles, codes, low, high):
    keys = []
    for h, tile in enumerate(tiles):
        k = unpacked(tile)
        code = codes[:, h * LANES : (h + 1) * LANES]
        is_low, is_high = code & 3, (code >> 2) & 3
        over = (code < 16) | ((is_high > 0) & (k >= high + is_high - 1))
        under = (is_low > 0) & (k < low + is_low - 1)
        keys.append(jnp.where(over, BIG, jnp.where(under, -1, k)))
    return keys


def place_kernel(found_ref, keys_out, values_out, size_out, digest_out):
    found = [found_ref[n * SUBS : (n + 1) * SUBS, :] for n in range(6)]
    keys, values, ranks = found[:2], found[2:4], found[4:]
    valid = sum(jnp.where((k >= 0) & (k < BIG), 1, 0) for k in keys)
    size = jnp.sum(jnp.sum(valid, axis=1, keepdims=True), axis=0, keepdims=True)
    count = 2 * SUBS
    keys, values = placed(
        list(zip(keys, values)), [r >> 7 for r in ranks], [r & (LANES - 1) for r in ranks], count
    )
    rank = iota((count, LANES), 0) * LANES + iota((count, LANES), 1)
    filled = rank < size
    keys = jnp.where(filled, keys, -1)
    values = jnp.where(filled, values, -1)
    keys_out[...] = keys[: keys_out.shape[0], :]
    values_out[...] = values[: values_out.shape[0], :]
    mixed = (keys + 3 * values + 5 * rank) & 1023
    digest = jnp.where(filled, 2 * mixed - 1023, 0)
    digest = jnp.sum(jnp.sum(digest, axis=1, keepdims=True), axis=0, keepdims=True)
    size_out[0] = size[0, 0]
    digest_out[0] = digest[0, 0]


def candidates(keys, values):
    dma = pltpu.SemaphoreType.DMA
    return pl.pallas_call(
        gather_kernel,
        out_shape=jax.ShapeDtypeStruct((6 * SUBS, LANES), i32),
        in_specs=[pl.BlockSpec(memory_space=pltpu.HBM)] * 2,
        out_specs=pl.BlockSpec(memory_space=pltpu.VMEM),
        scratch_shapes=[
            pltpu.VMEM((2, SUBS, LANES), i32),
            pltpu.VMEM((1, LANES), i32),
            pltpu.VMEM((2, SHORT, LANES), i32),
            pltpu.VMEM((LANES, 1, LANES), i32),
            pltpu.VMEM((2, LANES, SHORT, LANES), i32),
            pltpu.VMEM((LANES, LANES), i32),
            pltpu.VMEM((2, LANES, LANES), i32),
            dma((2,)),
            dma,
            dma,
            dma,
            dma,
            dma((2,)),
            dma((2, AXIS)),
            dma((2, AXIS)),
            dma((2, AXIS)),
        ],
        compiler_params=pltpu.CompilerParams(collective_id=0, has_side_effects=True, vmem_limit_bytes=8 << 20),
        name="find_candidates",
    )(keys, values)


def placed_bucket(found, rows):
    one = jax.ShapeDtypeStruct((1,), i32)
    return pl.pallas_call(
        place_kernel,
        out_shape=(jax.ShapeDtypeStruct((rows, LANES), i32),) * 2 + (one, one),
        in_specs=[pl.BlockSpec(memory_space=pltpu.VMEM)],
        out_specs=[pl.BlockSpec(memory_space=pltpu.VMEM)] * 2 + [pl.BlockSpec(memory_space=pltpu.SMEM)] * 2,
        compiler_params=pltpu.CompilerParams(vmem_limit_bytes=8 << 20),
        name="place_bucket",
    )(found)


def solution(mesh):
    gx, gy = mesh.shape["gx"], mesh.shape["gy"]

    def shards(record_keys, payloads):
        keys = record_keys.reshape(SUBS, LANES)
        values = payloads.reshape(SUBS, LANES)
        keys, values = (pltpu.with_memory_space_constraint(a, pltpu.HBM) for a in (keys, values))
        found = candidates(keys, values)
        rows = (2 * record_keys.shape[0] - gx * gy) // LANES
        sorted_keys, sorted_values, size, digest = placed_bucket(found, rows)
        return sorted_keys.reshape(-1), sorted_values.reshape(-1), size, digest

    spec = P(("gx", "gy"))
    return jax.shard_map(shards, mesh=mesh, in_specs=(spec,) * 2, out_specs=(spec,) * 4, check_vma=False)
```
